256 devices in a mesh: fsdp: 64 (over z, y, core), rep: 4 (over x).
Axes of the slice: x: 4, y: 4, z: 8, core: 2. Of those that a mesh axis runs over, the one named last changes fastest.
Arguments:
- partial_grad: bfloat16 [4, 64, 1024, 1024], P('rep', None, 'fsdp'), may hold values from -3 to 3
- owner_table: int32 [64, 2], replicated, may hold values from -1 to 63, as said below
- left_stat: float32 [64, 2, 1024, 1024], P('fsdp', None, None, 'rep'), may hold values from -6 to 6
- right_stat: float32 [64, 2, 1024, 1024], P('fsdp', None, None, 'rep'), may hold values from -6 to 6
- left_root: bfloat16 [64, 2, 1024, 1024], P('fsdp', None, None, 'rep'), may hold values from -0.1875 to 0.1875
- right_root: bfloat16 [64, 2, 1024, 1024], P('fsdp', None, None, 'rep'), may hold values from -0.1875 to 0.1875
Outputs:
- left_new: float32 [64, 2, 1024, 1024], P('fsdp', None, None, 'rep')
- right_new: float32 [64, 2, 1024, 1024], P('fsdp', None, None, 'rep')
- update: bfloat16 [64, 1024, 1024], P(None, 'fsdp', 'rep')
The draws below stay inside these ranges and needn't reach their ends.
Inputs may be any that keep to these rules, and one draw needn't show every extreme that they name: `owner_table`: each of the 64 blocks stands in exactly one slot and -1 marks an empty slot; some owner fills all 2 slots and some owner has none.
All inputs are finite; a program needn't handle non-finite values.
Results may differ from the reference program's by a relative error of at most 0.014.
Values may be sent and summed in bfloat16 or wider, within the bound.
A program may use at most 64 MiB of HBM per device.

```python
import jax
import jax.numpy as jnp
from jax import lax

BS = 1024
SLOTS = 2
BLOCKS = 64
N_FSDP = 64
N_REP = 4


def draw_owner_table(key, part):
    owners = BLOCKS
    first_key, second_key, third_key = jax.random.split(jax.random.fold_in(key, 7), 3)
    order = jax.random.permutation(first_key, owners).astype(jnp.int32)
    ranking = jnp.zeros((owners,), jnp.int32).at[order].set(jnp.arange(owners, dtype=jnp.int32))
    doubled = jax.random.randint(second_key, (), max(1, owners // 4), owners // 2 + 1).astype(jnp.int32)
    loads = jnp.where(ranking < doubled, 2, jnp.where(ranking < 2 * doubled, 0, 1)).astype(jnp.int32)
    filled = jnp.stack([loads >= 1, loads >= 2], axis=1).reshape(-1)
    counter = jnp.cumsum(filled.astype(jnp.int32)) - 1
    shuffled = jax.random.permutation(third_key, owners).astype(jnp.int32)
    picked = jnp.take(shuffled, jnp.maximum(counter, 0))
    return jnp.where(filled, picked, -1).astype(jnp.int32).reshape(owners, SLOTS)


def shard_levels(key, shape, cuts, least, largest):
    factor_of, own = 1.0, jax.random.fold_in(key, 6)
    for axis_at, blocks in cuts:
        heights = jnp.exp(jax.random.uniform(jax.random.fold_in(own, axis_at), (blocks,), jnp.float32, least / len(cuts), largest / len(cuts)))
        factor_of = factor_of * jnp.repeat(heights, shape[axis_at] // blocks).reshape([-1 if axis == axis_at else 1 for axis in range(len(shape))])
    return factor_of


def noise(own_key, dims, deviation, limit, pieces=(), kind=jnp.bfloat16):
    values = deviation * jax.random.normal(own_key, dims, jnp.float32)
    if pieces:
        values = values * shard_levels(own_key, dims, pieces, -0.22, 0.18)
    return jnp.clip(values, -limit, limit).astype(kind)


def setup_inputs(seed: int = 0) -> dict:
    key_of = jax.random.split(jax.random.key(seed), 7)
    return {
        "partial_grad": noise(key_of[0], (N_REP, BLOCKS, BS, BS), 0.5, 3.0, ((0, 4), (2, 64))),
        "owner_table": draw_owner_table(jax.random.fold_in(key_of[6], 71), 0),
        "left_stat": noise(key_of[2], (N_FSDP, SLOTS, BS, BS), 1.0, 6.0, ((0, 64), (3, 4)), jnp.float32),
        "right_stat": noise(key_of[3], (N_FSDP, SLOTS, BS, BS), 1.0, 6.0, ((0, 64), (3, 4)), jnp.float32),
        "left_root": noise(key_of[4], (N_FSDP, SLOTS, BS, BS), BS ** -0.5, 0.1875, ((0, 64), (3, 4))),
        "right_root": noise(key_of[5], (N_FSDP, SLOTS, BS, BS), BS ** -0.5, 0.1875, ((0, 64), (3, 4))),
    }


decay_rate = 0.99


def one_slot(summed, inputs):
    block_index, is_filled, left_old, right_old, left_inv, right_inv = inputs
    picked = lax.dynamic_index_in_dim(summed, block_index, 0, keepdims=False)
    slot_grad = jnp.where(is_filled, picked, jnp.zeros((), jnp.bfloat16))
    left_term = jnp.dot(slot_grad, slot_grad.T, preferred_element_type=jnp.float32)
    right_term = jnp.dot(slot_grad.T, slot_grad, preferred_element_type=jnp.float32)
    left_next = jnp.where(is_filled, decay_rate * left_old + (1.0 - decay_rate) * left_term, left_old)
    right_next = jnp.where(is_filled, decay_rate * right_old + (1.0 - decay_rate) * right_term, right_old)
    applied = jnp.dot(left_inv, slot_grad, preferred_element_type=jnp.float32).astype(jnp.bfloat16)
    result = jnp.dot(applied, right_inv, preferred_element_type=jnp.float32).astype(jnp.bfloat16)
    return left_next, right_next, result


def reference(partial_grad, owner_table, left_stat, right_stat, left_root, right_root):
    summed = jnp.sum(partial_grad.astype(jnp.float32), axis=0).astype(jnp.bfloat16)
    flat_table = owner_table.reshape(-1)
    filled_flat = flat_table >= 0
    index_flat = jnp.maximum(flat_table, 0).astype(jnp.int32)
    order = BS
    stacked = (index_flat, filled_flat, left_stat.reshape(-1, order, order), right_stat.reshape(-1, order, order), left_root.reshape(-1, order, order), right_root.reshape(-1, order, order))
    left_all, right_all, result_all = lax.map(lambda inputs: one_slot(summed, inputs), stacked)
    slot_ids = jnp.arange(flat_table.shape[0], dtype=jnp.int32)
    block_ids = jnp.arange(BLOCKS, dtype=jnp.int32)
    positions = jnp.sum(jnp.where(flat_table[None, :] == block_ids[:, None], slot_ids[None, :], 0), axis=1).astype(jnp.int32)
    update = jnp.take(result_all, positions, axis=0)
    return left_all.reshape(left_stat.shape), right_all.reshape(right_stat.shape), update
```

```python
import jax
import jax.numpy as jnp
from jax import lax
from jax.experimental import pallas as pl
from jax.experimental.pallas import tpu as pltpu
from jax.sharding import PartitionSpec as P

decay_rate = 0.99

NZ = 8
NY = 8
NX = 4
BLOCKS = 64
HALF = BLOCKS // 2
ROWS = 16
LANES = 128
BS = 1024
SHARE = 256
Z_STEPS = (4, 3, 5, 2, 6, 1, 7)
Y_STEPS = (4, 5, 2, 3, 6, 7, 1)
CHUNK_STEPS = Z_STEPS + (0,)
CHUNKS = 2 * NZ
EARLY = 4
AHEAD = 3


def lanes(index, width):
    return pl.ds(pl.multiple_of(index * width, width), width)


def wait_for(ref, sem):
    pltpu.make_async_copy(ref, ref, sem).wait()


def send(src, dst, send_sem, recv_sem, device):
    pltpu.make_async_remote_copy(
        src_ref=src,
        dst_ref=dst,
        send_sem=send_sem,
        recv_sem=recv_sem,
        device_id=device,
        device_id_type=pl.DeviceIdType.MESH,
    ).start()


def f32(x):
    return x.astype(jnp.float32)


def kernel(
    table, positions, grad, left, right,
    left_out, right_out, update_out,
    gv, relay_p, relay_m, near_p, near_m, far_p, far_m, shares,
    picked, landed, G, L, R, T, U, back, home, left_term, right_term,
    local_sem, rs_s, rs_r, z_s, z_r, y_s, y_r, g_s, g_r, l_s, l_r, bz_s, bz_r, by_s, by_r,
):
    f = lax.axis_index("fsdp")
    x = lax.axis_index("rep")
    z = lax.div(f, NY)
    yc = lax.rem(f, NY)
    nxt = lax.rem(x + 1, NX)
    opp = lax.rem(x + 2, NX)
    prv = lax.rem(x + 3, NX)
    to_nxt = (f, nxt)
    to_prv = (f, prv)

    def z_peer(step):
        return lax.rem(z + step, NZ)

    def y_peer(step):
        return lax.rem(yc + step, NY)

    loads = []
    for k in range(2 * NX):
        loads.append(
            pltpu.make_async_copy(
                grad.at[:, :, pl.ds(k * LANES, LANES)], gv.at[k], local_sem.at[k]
            )
        )
    left_loads = []
    for s in range(2):
        left_loads.append(
            pltpu.make_async_copy(
                left.at[s], L.at[s, :, :, lanes(x, SHARE)], local_sem.at[8 + s]
            )
        )
    right_load = pltpu.make_async_copy(right, R, local_sem.at[10])
    for copy in loads + left_loads + [right_load]:
        copy.start()

    barrier = pltpu.get_barrier_semaphore()
    peers = [to_nxt, to_prv]
    peers += [(z_peer(d) * NY + yc, x) for d in range(1, NZ)]
    peers += [(z * NY + y_peer(d), x) for d in range(1, NY)]
    for peer in peers:
        pl.semaphore_signal(barrier, inc=1, device_id=peer, device_id_type=pl.DeviceIdType.MESH)
    pl.semaphore_wait(barrier, len(peers))

    for copy in loads:
        copy.wait()

    def rs_first(h):
        send(gv.at[opp * 2 + h, pl.ds(0, HALF)], relay_p.at[h], rs_s.at[h, 0], rs_r.at[h, 0], to_nxt)
        send(gv.at[opp * 2 + h, pl.ds(HALF, HALF)], relay_m.at[h], rs_s.at[h, 1], rs_r.at[h, 1], to_prv)
        send(gv.at[nxt * 2 + h, pl.ds(HALF, HALF)], near_p.at[h], rs_s.at[h, 2], rs_r.at[h, 2], to_nxt)
        send(gv.at[prv * 2 + h, pl.ds(0, HALF)], near_m.at[h], rs_s.at[h, 3], rs_r.at[h, 3], to_prv)

    def rs_second(h):
        wait_for(relay_p.at[h], rs_r.at[h, 0])
        relay_p[h] = (f32(relay_p[h]) + f32(gv[nxt * 2 + h, pl.ds(0, HALF)])).astype(jnp.bfloat16)
        send(relay_p.at[h], far_p.at[h], rs_s.at[h, 4], rs_r.at[h, 4], to_nxt)
        wait_for(relay_m.at[h], rs_r.at[h, 1])
        relay_m[h] = (f32(relay_m[h]) + f32(gv[prv * 2 + h, pl.ds(HALF, HALF)])).astype(jnp.bfloat16)
        send(relay_m.at[h], far_m.at[h], rs_s.at[h, 5], rs_r.at[h, 5], to_prv)

    def rs_final(h):
        wait_for(near_p.at[h], rs_r.at[h, 2])
        wait_for(near_m.at[h], rs_r.at[h, 3])
        wait_for(far_p.at[h], rs_r.at[h, 4])
        wait_for(far_m.at[h], rs_r.at[h, 5])
        own = x * 2 + h
        low = f32(gv[own, pl.ds(0, HALF)]) + f32(near_m[h]) + f32(far_p[h])
        shares[h, pl.ds(0, HALF)] = low.astype(jnp.bfloat16)
        high = f32(gv[own, pl.ds(HALF, HALF)]) + f32(near_p[h]) + f32(far_m[h])
        shares[h, pl.ds(HALF, HALF)] = high.astype(jnp.bfloat16)

        def pick(owner, carry):
            for s in range(2):
                block = table[owner, s]
                value = shares[h, jnp.maximum(block, 0)]
                picked[h, s, owner] = jnp.where(block >= 0, value, jnp.zeros_like(value))
            return carry

        lax.fori_loop(0, NZ * NY, pick, 0, unroll=8)

    def z_send(h, s):
        for d in Z_STEPS:
            zp = z_peer(d)
            send(
                picked.at[h, s, pl.ds(zp * NY, NY)], landed.at[h, s, z],
                z_s.at[h, s], z_r.at[h, s], (zp * NY + yc, x),
            )
        landed[h, s, z] = picked[h, s, pl.ds(z * NY, NY)]

    def y_send(h, s):
        wait_for(landed.at[h, s, pl.ds(0, NZ - 1)], z_r.at[h, s])
        where = lanes(x * 2 + h, LANES)
        for d in Y_STEPS:
            yp = y_peer(d)
            send(
                landed.at[h, s, :, yp], G.at[s, :, yc, :, where],
                y_s.at[h, s], y_r.at[h, s], (z * NY + yp, x),
            )
        G[s, :, yc, :, where] = landed[h, s, :, yc]

    def g_send(h, s):
        where = lanes(x * 2 + h, LANES)
        wait_for(G.at[s, :, pl.ds(0, NY - 1), :, where], y_r.at[h, s])
        mine = G.at[s, :, :, :, where]
        send(mine, mine, g_s.at[h, s, 0], g_r.at[h, s, 0], to_nxt)
        send(mine, mine, g_s.at[h, s, 1], g_r.at[h, s, 1], to_prv)

    def g_relay(h, s):
        from_prv = lanes(prv * 2 + h, LANES)
        wait_for(G.at[s, :, :, :, from_prv], g_r.at[h, s, 0])
        part = G.at[s, pl.ds(0, NZ // 2), :, :, from_prv]
        send(part, part, g_s.at[h, s, 2], g_r.at[h, s, 2], to_nxt)
        from_nxt = lanes(nxt * 2 + h, LANES)
        wait_for(G.at[s, :, :, :, from_nxt], g_r.at[h, s, 1])
        part = G.at[s, pl.ds(NZ // 2, NZ // 2), :, :, from_nxt]
        send(part, part, g_s.at[h, s, 3], g_r.at[h, s, 3], to_prv)

    def g_done(h, s):
        where = lanes(opp * 2 + h, LANES)
        wait_for(G.at[s, pl.ds(0, NZ // 2), :, :, where], g_r.at[h, s, 2])
        wait_for(G.at[s, pl.ds(NZ // 2, NZ // 2), :, :, where], g_r.at[h, s, 3])

    def chunk(c):
        return c // NZ, z_peer(CHUNK_STEPS[c % NZ])

    def l_send(c):
        s, zc = chunk(c)
        mine = L.at[s, zc, :, lanes(x, SHARE)]
        send(mine, mine, l_s.at[c, 0], l_r.at[c, 0], to_nxt)
        send(mine, mine, l_s.at[c, 1], l_r.at[c, 1], to_prv)

    def l_relay(c):
        s, zc = chunk(c)
        wait_for(L.at[s, zc, :, lanes(prv, SHARE)], l_r.at[c, 0])
        part = L.at[s, zc, pl.ds(0, LANES // 2), lanes(prv, SHARE)]
        send(part, part, l_s.at[c, 2], l_r.at[c, 2], to_nxt)
        wait_for(L.at[s, zc, :, lanes(nxt, SHARE)], l_r.at[c, 1])
        part = L.at[s, zc, pl.ds(LANES // 2, LANES // 2), lanes(nxt, SHARE)]
        send(part, part, l_s.at[c, 3], l_r.at[c, 3], to_prv)

    def right_product(s):
        @pl.loop(0, NZ // 2)
        def _(i):
            rows = G[s, pl.ds(i * 2, 2)].reshape(SHARE, BS)
            result = jnp.dot(rows, R[s], preferred_element_type=jnp.float32)
            T[s, pl.ds(pl.multiple_of(i * SHARE, SHARE), SHARE), :] = result.astype(jnp.bfloat16)

    def left_statistic(s):
        mine = G[s, pl.ds(x * 2, 2)].reshape(SHARE, BS)

        @pl.loop(0, NZ // 2)
        def _(i):
            rows = G[s, pl.ds(i * 2, 2)].reshape(SHARE, BS)
            result = lax.dot_general(
                rows, mine, (((1,), (1,)), ((), ())), preferred_element_type=jnp.float32
            )
            left_term[s, pl.ds(pl.multiple_of(i * SHARE, SHARE), SHARE), :] = result.astype(jnp.bfloat16)

        pltpu.make_async_copy(left_term.at[s], left_out.at[s], local_sem.at[11 + s]).start()

    def right_statistic(s):
        @pl.loop(0, NX)
        def _(i):
            columns = G[s, :, :, :, lanes(i, SHARE)].reshape(BS, SHARE)
            mine = G[s, :, :, :, lanes(x, SHARE)].reshape(BS, SHARE)
            result = lax.dot_general(
                columns, mine, (((0,), (0,)), ((), ())), preferred_element_type=jnp.float32
            )
            right_term[s, pl.ds(pl.multiple_of(i * SHARE, SHARE), SHARE), :] = result.astype(jnp.bfloat16)

        pltpu.make_async_copy(right_term.at[s], right_out.at[s], local_sem.at[13 + s]).start()

    def update_chunk(c):
        s, zc = chunk(c)
        wait_for(L.at[s, zc, pl.ds(0, LANES // 2), lanes(opp, SHARE)], l_r.at[c, 2])
        wait_for(L.at[s, zc, pl.ds(LANES // 2, LANES // 2), lanes(opp, SHARE)], l_r.at[c, 3])
        result = jnp.dot(L[s, zc], T[s], preferred_element_type=jnp.float32)
        U[s, zc] = result.astype(jnp.bfloat16).reshape(NY, ROWS, SHARE)
        if CHUNK_STEPS[c % NZ] == 0:
            back[s, z] = U[s, z]
        else:
            send(U.at[s, zc], back.at[s, z], bz_s.at[s], bz_r.at[s], (zc * NY + yc, x))

    def back_send(s):
        wait_for(back.at[s, pl.ds(0, NZ - 1)], bz_r.at[s])
        place = pl.ds(s * NZ * NY + yc * NZ, NZ)
        for d in Y_STEPS:
            yp = y_peer(d)
            send(back.at[s, :, yp], home.at[place], by_s.at[s], by_r.at[s], (z * NY + yp, x))
        home[place] = back[s, :, yc]

    rs_first(0)
    rs_second(0)
    rs_first(1)
    rs_final(0)
    z_send(0, 0)
    z_send(0, 1)
    rs_second(1)
    for copy in left_loads:
        copy.wait()
    for c in range(EARLY):
        l_send(c)
    rs_final(1)
    z_send(1, 0)
    z_send(1, 1)
    y_send(0, 0)
    l_relay(0)
    l_relay(1)
    y_send(0, 1)
    g_send(0, 0)
    l_relay(2)
    l_relay(3)
    y_send(1, 0)
    g_send(0, 1)
    g_relay(0, 0)
    y_send(1, 1)
    g_send(1, 0)
    g_relay(0, 1)
    g_send(1, 1)
    g_relay(1, 0)
    for c in range(EARLY, EARLY + AHEAD):
        l_send(c)
    right_load.wait()
    g_done(0, 0)
    g_done(1, 0)
    right_product(0)
    g_relay(1, 1)
    for c in range(EARLY, CHUNKS):
        if c + AHEAD < CHUNKS:
            l_send(c + AHEAD)
        l_relay(c)
        if c == EARLY:
            for early in range(EARLY - 1):
                update_chunk(early)
        if c == EARLY + 1:
            g_done(0, 1)
            g_done(1, 1)
            right_product(1)
        if c == EARLY + 2:
            left_statistic(0)
        if c == EARLY + 3:
            right_statistic(0)
        if c == EARLY + 5:
            left_statistic(1)
        if c == EARLY + 6:
            right_statistic(1)
        update_chunk(c - 1)
        if c == NZ + 2:
            back_send(0)
    update_chunk(CHUNKS - 1)
    back_send(1)
    for s in range(2):
        wait_for(home.at[pl.ds(s * NZ * NY, (NY - 1) * NZ)], by_r.at[s])

    def place_block(b, carry):
        update_out[b] = home[positions[b]]
        return carry

    lax.fori_loop(0, BLOCKS, place_block, 0, unroll=8)

    for h in range(2):
        for k, ref in enumerate((relay_p, relay_m, near_p, near_m, far_p, far_m)):
            wait_for(ref.at[h], rs_s.at[h, k])
        for s in range(2):
            where = lanes(x * 2 + h, LANES)
            wait_for(picked.at[h, s, pl.ds(0, (NZ - 1) * NY)], z_s.at[h, s])
            wait_for(landed.at[h, s, :, pl.ds(0, NY - 1)], y_s.at[h, s])
            for k in range(2):
                wait_for(G.at[s, :, :, :, where], g_s.at[h, s, k])
                wait_for(G.at[s, pl.ds(0, NZ // 2), :, :, where], g_s.at[h, s, 2 + k])
    for c in range(CHUNKS):
        s, zc = chunk(c)
        for k in range(2):
            wait_for(L.at[s, zc, :, lanes(x, SHARE)], l_s.at[c, k])
            wait_for(L.at[s, zc, pl.ds(0, LANES // 2), lanes(x, SHARE)], l_s.at[c, 2 + k])
    for s in range(2):
        wait_for(U.at[s, pl.ds(0, NZ - 1)], bz_s.at[s])
        wait_for(back.at[s, :, pl.ds(0, NY - 1)], by_s.at[s])
        pltpu.make_async_copy(left_term.at[s], left_out.at[s], local_sem.at[11 + s]).wait()
        pltpu.make_async_copy(right_term.at[s], right_out.at[s], local_sem.at[13 + s]).wait()


def exchange(table, positions, grad, left, right):
    bf16 = jnp.bfloat16
    any_spec = pl.BlockSpec(memory_space=pl.ANY)
    smem_spec = pl.BlockSpec(memory_space=pltpu.SMEM)
    dma = pltpu.SemaphoreType.DMA
    half = (2, HALF, ROWS, LANES)
    return pl.pallas_call(
        kernel,
        name="shampoo_exchange",
        out_shape=(
            jax.ShapeDtypeStruct((2, BS, SHARE), bf16),
            jax.ShapeDtypeStruct((2, BS, SHARE), bf16),
            jax.ShapeDtypeStruct((BLOCKS, ROWS, SHARE), bf16),
        ),
        in_specs=[smem_spec, smem_spec, any_spec, any_spec, any_spec],
        out_specs=(any_spec, any_spec, pl.BlockSpec(memory_space=pltpu.VMEM)),
        scratch_shapes=[
            pltpu.VMEM((2 * NX, BLOCKS, ROWS, LANES), bf16),
            pltpu.VMEM(half, bf16),
            pltpu.VMEM(half, bf16),
            pltpu.VMEM(half, bf16),
            pltpu.VMEM(half, bf16),
            pltpu.VMEM(half, bf16),
            pltpu.VMEM(half, bf16),
            pltpu.VMEM((2, BLOCKS, ROWS, LANES), bf16),
            pltpu.VMEM((2, 2, NZ * NY, ROWS, LANES), bf16),
            pltpu.VMEM((2, 2, NZ, NY, ROWS, LANES), bf16),
            pltpu.VMEM((2, NZ, NY, ROWS, BS), bf16),
            pltpu.VMEM((2, NZ, LANES, BS), bf16),
            pltpu.VMEM((2, BS, SHARE), bf16),
            pltpu.VMEM((2, BS, SHARE), bf16),
            pltpu.VMEM((2, NZ, NY, ROWS, SHARE), bf16),
            pltpu.VMEM((2, NZ, NY, ROWS, SHARE), bf16),
            pltpu.VMEM((2 * NZ * NY, ROWS, SHARE), bf16),
            pltpu.VMEM((2, BS, SHARE), bf16),
            pltpu.VMEM((2, BS, SHARE), bf16),
            dma((15,)),
            dma((2, 6)),
            dma((2, 6)),
            dma((2, 2)),
            dma((2, 2)),
            dma((2, 2)),
            dma((2, 2)),
            dma((2, 2, 4)),
            dma((2, 2, 4)),
            dma((CHUNKS, 4)),
            dma((CHUNKS, 4)),
            dma((2,)),
            dma((2,)),
            dma((2,)),
            dma((2,)),
        ],
        compiler_params=pltpu.CompilerParams(
            collective_id=0, has_side_effects=True, vmem_limit_bytes=56 * 1024 * 1024
        ),
        cost_estimate=pl.CostEstimate(
            flops=16 * BS * BS * SHARE, bytes_accessed=16 * BS * BS, transcendentals=0
        ),
    )(table, positions, grad, left, right)


def on_device(partial_grad, owner_table, left_stat, right_stat, left_root, right_root):
    filled = lax.dynamic_index_in_dim(owner_table, lax.axis_index("fsdp"), 0, keepdims=False) >= 0
    flat = owner_table.reshape(NZ, NY, 2).transpose(2, 1, 0).reshape(-1)
    slot_ids = jnp.arange(2 * NZ * NY, dtype=jnp.int32)
    block_ids = jnp.arange(BLOCKS, dtype=jnp.int32)
    positions = jnp.sum(jnp.where(flat[None, :] == block_ids[:, None], slot_ids[None, :], 0), axis=1)
    left_term, right_term, update = exchange(
        owner_table,
        positions,
        partial_grad[0],
        left_root[0].reshape(2, NZ, LANES, SHARE),
        right_root[0],
    )
    keeper = filled[:, None, None]

    def next_of(stat, term):
        moved = decay_rate * stat + (1.0 - decay_rate) * term.astype(jnp.float32)
        return jnp.where(keeper, moved, stat)

    return (
        next_of(left_stat[0], left_term)[None],
        next_of(right_stat[0], right_term)[None],
        update,
    )


def solution(mesh):
    return jax.shard_map(
        on_device,
        mesh=mesh,
        in_specs=(
            P("rep", None, "fsdp", None),
            P(),
            P("fsdp", None, None, "rep"),
            P("fsdp", None, None, "rep"),
            P("fsdp", None, None, "rep"),
            P("fsdp", None, None, "rep"),
        ),
        out_specs=(
            P("fsdp", None, None, "rep"),
            P("fsdp", None, None, "rep"),
            P(None, "fsdp", "rep"),
        ),
        check_vma=False,
    )
```

```python
import jax
import jax.numpy as jnp
from jax import lax
from jax.experimental import pallas as pl
from jax.experimental.pallas import tpu as pltpu
from jax.sharding import PartitionSpec as P

decay_rate = 0.99

NZ = 8
NY = 8
NX = 4
BLOCKS = 64
HALF = BLOCKS // 2
ROWS = 16
LANES = 128
BS = 1024
SHARE = 256
Z_STEPS = (4, 3, 5, 2, 6, 1, 7)
Y_STEPS = (4, 5, 2, 3, 6, 7, 1)
CHUNK_ORDER = (
    (0, 4), (0, 3), (0, 5), (0, 2), (0, 6), (0, 1), (0, 7), (1, 4),
    (1, 3), (1, 5), (1, 2), (1, 6), (1, 1), (1, 7), (0, 0), (1, 0),
)
CHUNKS = len(CHUNK_ORDER)


def lanes(index, width):
    return pl.ds(pl.multiple_of(index * width, width), width)


def wait_for(ref, sem):
    pltpu.make_async_copy(ref, ref, sem).wait()


def send(src, dst, send_sem, recv_sem, device):
    pltpu.make_async_remote_copy(
        src_ref=src,
        dst_ref=dst,
        send_sem=send_sem,
        recv_sem=recv_sem,
        device_id=device,
        device_id_type=pl.DeviceIdType.MESH,
    ).start()


def f32(x):
    return x.astype(jnp.float32)


def kernel(
    table_hbm, grad, left, right,
    left_out, right_out, update_out, keep_out,
    table, table_v, positions, positions_v, gv, relay_p, relay_m, near_p, near_m, far_p, far_m, shares,
    picked, landed, G, L, R, T, U, back, home, left_term, right_term,
    local_sem, rs_s, rs_r, z_s, z_r, y_s, y_r, g_s, g_r, l_s, l_r, bz_s, bz_r, by_s, by_r,
):
    f = lax.axis_index("fsdp")
    x = lax.axis_index("rep")
    z = lax.div(f, NY)
    yc = lax.rem(f, NY)
    nxt = lax.rem(x + 1, NX)
    opp = lax.rem(x + 2, NX)
    prv = lax.rem(x + 3, NX)
    to_nxt = (f, nxt)
    to_prv = (f, prv)

    def z_peer(step):
        return lax.rem(z + step, NZ)

    def y_peer(step):
        return lax.rem(yc + step, NY)

    barrier = pltpu.get_barrier_semaphore()
    peers = [(z_peer(d) * NY + yc, x) for d in Z_STEPS]
    peers += [(z * NY + y_peer(d), x) for d in Y_STEPS]
    peers += [to_nxt, to_prv]
    for peer in peers:
        pl.semaphore_signal(barrier, inc=1, device_id=peer, device_id_type=pl.DeviceIdType.MESH)
    loads = []
    for k in range(2 * NX):
        loads.append(
            pltpu.make_async_copy(
                grad.at[:, :, pl.ds(k * LANES, LANES)], gv.at[k], local_sem.at[k]
            )
        )
    left_loads = []
    for s in range(2):
        left_loads.append(
            pltpu.make_async_copy(
                left.at[s], L.at[s, :, :, lanes(x, SHARE)], local_sem.at[8 + s]
            )
        )
    right_load = pltpu.make_async_copy(right, R, local_sem.at[10])
    table_loads = [
        pltpu.make_async_copy(table_hbm, table, local_sem.at[15]),
        pltpu.make_async_copy(table_hbm, table_v, local_sem.at[16]),
    ]
    for copy in loads + table_loads + left_loads + [right_load]:
        copy.start()

    pl.semaphore_wait(barrier, len(peers))

    for copy in loads:
        copy.wait()

    def rs_first(h):
        send(gv.at[opp * 2 + h, pl.ds(0, HALF)], relay_p.at[h], rs_s.at[h, 0], rs_r.at[h, 0], to_nxt)
        send(gv.at[opp * 2 + h, pl.ds(HALF, HALF)], relay_m.at[h], rs_s.at[h, 1], rs_r.at[h, 1], to_prv)
        send(gv.at[nxt * 2 + h, pl.ds(HALF, HALF)], near_p.at[h], rs_s.at[h, 2], rs_r.at[h, 2], to_nxt)
        send(gv.at[prv * 2 + h, pl.ds(0, HALF)], near_m.at[h], rs_s.at[h, 3], rs_r.at[h, 3], to_prv)

    def rs_second(h):
        wait_for(relay_p.at[h], rs_r.at[h, 0])
        relay_p[h] = (f32(relay_p[h]) + f32(gv[nxt * 2 + h, pl.ds(0, HALF)])).astype(jnp.bfloat16)
        send(relay_p.at[h], far_p.at[h], rs_s.at[h, 4], rs_r.at[h, 4], to_nxt)
        wait_for(relay_m.at[h], rs_r.at[h, 1])
        relay_m[h] = (f32(relay_m[h]) + f32(gv[prv * 2 + h, pl.ds(HALF, HALF)])).astype(jnp.bfloat16)
        send(relay_m.at[h], far_m.at[h], rs_s.at[h, 5], rs_r.at[h, 5], to_prv)

    def rs_final(h):
        wait_for(near_p.at[h], rs_r.at[h, 2])
        wait_for(near_m.at[h], rs_r.at[h, 3])
        wait_for(far_p.at[h], rs_r.at[h, 4])
        wait_for(far_m.at[h], rs_r.at[h, 5])
        own = x * 2 + h
        low = f32(gv[own, pl.ds(0, HALF)]) + f32(near_m[h]) + f32(far_p[h])
        shares[h, pl.ds(0, HALF)] = low.astype(jnp.bfloat16)
        high = f32(gv[own, pl.ds(HALF, HALF)]) + f32(near_p[h]) + f32(far_m[h])
        shares[h, pl.ds(HALF, HALF)] = high.astype(jnp.bfloat16)

        def pick(owner, carry):
            for s in range(2):
                block = table[s, owner]
                value = shares[h, jnp.maximum(block, 0)]
                picked[h, s, owner] = jnp.where(block >= 0, value, jnp.zeros_like(value))
            return carry

        lax.fori_loop(0, NZ * NY, pick, 0, unroll=8)

    def z_send(h, s):
        for d in Z_STEPS:
            zp = z_peer(d)
            send(
                picked.at[h, s, pl.ds(zp * NY, NY)], landed.at[h, s, z],
                z_s.at[h, s], z_r.at[h, s], (zp * NY + yc, x),
            )
        landed[h, s, z] = picked[h, s, pl.ds(z * NY, NY)]

    def y_send(h, s):
        wait_for(landed.at[h, s, pl.ds(0, NZ - 1)], z_r.at[h, s])
        where = lanes(x * 2 + h, LANES)
        for d in Y_STEPS:
            yp = y_peer(d)
            send(
                landed.at[h, s, :, yp], G.at[s, :, yc, :, where],
                y_s.at[h, s], y_r.at[h, s], (z * NY + yp, x),
            )
        G[s, :, yc, :, where] = landed[h, s, :, yc]

    def g_send(h, s):
        where = lanes(x * 2 + h, LANES)
        wait_for(G.at[s, :, pl.ds(0, NY - 1), :, where], y_r.at[h, s])
        mine = G.at[s, :, :, :, where]
        send(mine, mine, g_s.at[h, s, 0], g_r.at[h, s, 0], to_nxt)
        send(mine, mine, g_s.at[h, s, 1], g_r.at[h, s, 1], to_prv)

    def g_relay(h, s):
        from_prv = lanes(prv * 2 + h, LANES)
        wait_for(G.at[s, :, :, :, from_prv], g_r.at[h, s, 0])
        part = G.at[s, pl.ds(0, NZ // 2), :, :, from_prv]
        send(part, part, g_s.at[h, s, 2], g_r.at[h, s, 2], to_nxt)
        from_nxt = lanes(nxt * 2 + h, LANES)
        wait_for(G.at[s, :, :, :, from_nxt], g_r.at[h, s, 1])
        part = G.at[s, pl.ds(NZ // 2, NZ // 2), :, :, from_nxt]
        send(part, part, g_s.at[h, s, 3], g_r.at[h, s, 3], to_prv)

    def g_done(h, s):
        where = lanes(opp * 2 + h, LANES)
        wait_for(G.at[s, pl.ds(0, NZ // 2), :, :, where], g_r.at[h, s, 2])
        wait_for(G.at[s, pl.ds(NZ // 2, NZ // 2), :, :, where], g_r.at[h, s, 3])

    def chunk(c):
        s, step = CHUNK_ORDER[c]
        return s, z_peer(step)

    def l_send(c):
        s, zc = chunk(c)
        mine = L.at[s, zc, :, lanes(x, SHARE)]
        send(mine, mine, l_s.at[0], l_r.at[c, 0], to_nxt)
        send(mine, mine, l_s.at[1], l_r.at[c, 1], to_prv)

    def l_relay(c):
        s, zc = chunk(c)
        wait_for(L.at[s, zc, :, lanes(prv, SHARE)], l_r.at[c, 0])
        part = L.at[s, zc, pl.ds(0, LANES // 2), lanes(prv, SHARE)]
        send(part, part, l_s.at[2], l_r.at[c, 2], to_nxt)
        wait_for(L.at[s, zc, :, lanes(nxt, SHARE)], l_r.at[c, 1])
        part = L.at[s, zc, pl.ds(LANES // 2, LANES // 2), lanes(nxt, SHARE)]
        send(part, part, l_s.at[3], l_r.at[c, 3], to_prv)

    def right_product(s):
        @pl.loop(0, NZ // 2)
        def _(i):
            rows = G[s, pl.ds(i * 2, 2)].reshape(SHARE, BS)
            result = jnp.dot(rows, R[s], preferred_element_type=jnp.float32)
            T[s, pl.ds(pl.multiple_of(i * SHARE, SHARE), SHARE), :] = result.astype(jnp.bfloat16)

    def left_statistic(s):
        mine = G[s, pl.ds(x * 2, 2)].reshape(SHARE, BS)

        @pl.loop(0, NZ // 2)
        def _(i):
            rows = G[s, pl.ds(i * 2, 2)].reshape(SHARE, BS)
            result = lax.dot_general(
                rows, mine, (((1,), (1,)), ((), ())), preferred_element_type=jnp.float32
            )
            left_term[s, pl.ds(pl.multiple_of(i * SHARE, SHARE), SHARE), :] = result.astype(jnp.bfloat16)

        pltpu.make_async_copy(left_term.at[s], left_out.at[s], local_sem.at[11 + s]).start()

    def right_statistic(s):
        @pl.loop(0, NX)
        def _(i):
            columns = G[s, :, :, :, lanes(i, SHARE)].reshape(BS, SHARE)
            mine = G[s, :, :, :, lanes(x, SHARE)].reshape(BS, SHARE)
            result = lax.dot_general(
                columns, mine, (((0,), (0,)), ((), ())), preferred_element_type=jnp.float32
            )
            right_term[s, pl.ds(pl.multiple_of(i * SHARE, SHARE), SHARE), :] = result.astype(jnp.bfloat16)

        pltpu.make_async_copy(right_term.at[s], right_out.at[s], local_sem.at[13 + s]).start()

    def update_chunk(c):
        s, zc = chunk(c)
        wait_for(L.at[s, zc, pl.ds(0, LANES // 2), lanes(opp, SHARE)], l_r.at[c, 2])
        wait_for(L.at[s, zc, pl.ds(LANES // 2, LANES // 2), lanes(opp, SHARE)], l_r.at[c, 3])
        result = jnp.dot(L[s, zc], T[s], preferred_element_type=jnp.float32)
        U[s, zc] = result.astype(jnp.bfloat16).reshape(NY, ROWS, SHARE)
        if CHUNK_ORDER[c][1] == 0:
            back[s, z] = U[s, z]
        else:
            send(U.at[s, zc], back.at[s, z], bz_s.at[s], bz_r.at[c], (zc * NY + yc, x))

    def back_send(c):
        s, step = CHUNK_ORDER[c]
        source = lax.rem(z + NZ - step, NZ)
        if step != 0:
            wait_for(back.at[s, source], bz_r.at[c])
        place = s * NZ * NY + yc * NZ + source
        for d in Y_STEPS:
            yp = y_peer(d)
            send(back.at[s, source, yp], home.at[place], by_s.at[s], by_r.at[s], (z * NY + yp, x))
        home[place] = back[s, source, yc]

    def find_positions():
        table_loads[1].wait()
        total = jnp.zeros((1, LANES), jnp.int32)
        owner = lax.broadcasted_iota(jnp.int32, (NZ * NY, LANES), 0)
        block = lax.broadcasted_iota(jnp.int32, (NZ * NY, LANES), 1)
        slot = lax.rem(owner, NY) * NZ + lax.div(owner, NY)
        for s in range(2):
            row = table_v[pl.ds(s, 1), :]
            held = jnp.broadcast_to(row, (LANES, NZ * NY)).T
            hit = jnp.where(held == block, slot + s * NZ * NY, 0)
            total += jnp.sum(hit, axis=0, keepdims=True)
        positions_v[...] = jnp.minimum(total, 2 * NZ * NY - 1)
        copy = pltpu.make_async_copy(positions_v, positions, local_sem.at[17])
        copy.start()
        copy.wait()
        for s in range(2):
            factor = jnp.where(table[s, f] >= 0, decay_rate, 1.0).astype(jnp.float32)
            keep_out[s] = jnp.full((8, LANES), factor, jnp.float32)

    rs_first(0)
    left_loads[0].wait()
    l_send(0)
    rs_second(0)
    rs_first(1)
    l_send(1)
    table_loads[0].wait()
    rs_final(0)
    z_send(0, 0)
    rs_second(1)
    for c in range(2, 6):
        l_send(c)
    find_positions()
    rs_final(1)
    z_send(1, 0)
    z_send(0, 1)
    z_send(1, 1)
    y_send(0, 0)
    l_relay(0)
    l_relay(1)
    l_send(6)
    l_relay(2)
    l_relay(3)
    g_send(0, 0)
    l_relay(4)
    l_relay(5)
    y_send(1, 0)
    l_relay(6)
    g_send(1, 0)
    y_send(0, 1)
    g_relay(0, 0)
    g_send(0, 1)
    y_send(1, 1)
    g_relay(1, 0)
    g_send(1, 1)
    right_load.wait()
    left_loads[1].wait()
    g_relay(0, 1)
    l_send(7)
    g_done(0, 0)
    g_done(1, 0)
    right_product(0)
    for c in range(0, 7):
        update_chunk(c)
    left_statistic(0)
    g_relay(1, 1)
    l_send(8)
    l_send(9)
    l_send(10)
    right_statistic(0)
    l_relay(7)
    l_send(11)
    g_done(0, 1)
    g_done(1, 1)
    right_product(1)
    l_relay(8)
    l_send(12)
    left_statistic(1)
    l_relay(9)
    l_send(13)
    right_statistic(1)
    l_relay(10)
    l_send(14)
    update_chunk(7)
    l_relay(11)
    l_send(15)
    update_chunk(8)
    back_send(2)
    back_send(0)
    l_relay(12)
    update_chunk(9)
    back_send(4)
    back_send(1)
    l_relay(13)
    update_chunk(10)
    back_send(5)
    back_send(3)
    l_relay(14)
    update_chunk(11)
    l_relay(15)
    update_chunk(12)
    update_chunk(13)
    back_send(6)
    update_chunk(14)
    back_send(14)
    update_chunk(15)
    back_send(15)
    for c in range(7, 14):
        back_send(c)
    for h in range(2):
        for k, ref in enumerate((relay_p, relay_m, near_p, near_m, far_p, far_m)):
            wait_for(ref.at[h], rs_s.at[h, k])
        for s in range(2):
            where = lanes(x * 2 + h, LANES)
            wait_for(picked.at[h, s, pl.ds(0, (NZ - 1) * NY)], z_s.at[h, s])
            wait_for(landed.at[h, s, :, pl.ds(0, NY - 1)], y_s.at[h, s])
            for k in range(2):
                wait_for(G.at[s, :, :, :, where], g_s.at[h, s, k])
                wait_for(G.at[s, pl.ds(0, NZ // 2), :, :, where], g_s.at[h, s, 2 + k])
    for k in range(2):
        wait_for(L.at[:, :, :, lanes(x, SHARE)], l_s.at[k])
        wait_for(L.at[0, :, :, lanes(x, SHARE)], l_s.at[2 + k])
    for s in range(2):
        wait_for(U.at[s, pl.ds(0, NZ - 1)], bz_s.at[s])
        pltpu.make_async_copy(left_term.at[s], left_out.at[s], local_sem.at[11 + s]).wait()
        pltpu.make_async_copy(right_term.at[s], right_out.at[s], local_sem.at[13 + s]).wait()

    for s in range(2):
        wait_for(home.at[pl.ds(s * NZ * NY, (NY - 1) * NZ)], by_r.at[s])

    def place_block(b, carry):
        update_out[b] = home[positions[0, b]]
        return carry

    lax.fori_loop(0, BLOCKS, place_block, 0, unroll=8)

    for s in range(2):
        wait_for(back.at[s, :, pl.ds(0, NY - 1)], by_s.at[s])


def exchange(table, grad, left, right):
    bf16 = jnp.bfloat16
    any_spec = pl.BlockSpec(memory_space=pl.ANY)
    hbm_spec = pl.BlockSpec(memory_space=pltpu.HBM)
    vmem_spec = pl.BlockSpec(memory_space=pltpu.VMEM)
    dma = pltpu.SemaphoreType.DMA
    half = (2, HALF, ROWS, LANES)
    return pl.pallas_call(
        kernel,
        name="shampoo_exchange",
        out_shape=(
            jax.ShapeDtypeStruct((2, BS, SHARE), bf16),
            jax.ShapeDtypeStruct((2, BS, SHARE), bf16),
            jax.ShapeDtypeStruct((BLOCKS, ROWS, SHARE), bf16),
            jax.ShapeDtypeStruct((2, 8, LANES), jnp.float32),
        ),
        in_specs=[hbm_spec, hbm_spec, hbm_spec, hbm_spec],
        out_specs=(any_spec, any_spec, vmem_spec, vmem_spec),
        scratch_shapes=[
            pltpu.SMEM((2, NZ * NY), jnp.int32),
            pltpu.VMEM((2, NZ * NY), jnp.int32),
            pltpu.SMEM((1, LANES), jnp.int32),
            pltpu.VMEM((1, LANES), jnp.int32),
            pltpu.VMEM((2 * NX, BLOCKS, ROWS, LANES), bf16),
            pltpu.VMEM(half, bf16),
            pltpu.VMEM(half, bf16),
            pltpu.VMEM(half, bf16),
            pltpu.VMEM(half, bf16),
            pltpu.VMEM(half, bf16),
            pltpu.VMEM(half, bf16),
            pltpu.VMEM((2, BLOCKS, ROWS, LANES), bf16),
            pltpu.VMEM((2, 2, NZ * NY, ROWS, LANES), bf16),
            pltpu.VMEM((2, 2, NZ, NY, ROWS, LANES), bf16),
            pltpu.VMEM((2, NZ, NY, ROWS, BS), bf16),
            pltpu.VMEM((2, NZ, LANES, BS), bf16),
            pltpu.VMEM((2, BS, SHARE), bf16),
            pltpu.VMEM((2, BS, SHARE), bf16),
            pltpu.VMEM((2, NZ, NY, ROWS, SHARE), bf16),
            pltpu.VMEM((2, NZ, NY, ROWS, SHARE), bf16),
            pltpu.VMEM((2 * NZ * NY, ROWS, SHARE), bf16),
            pltpu.VMEM((2, BS, SHARE), bf16),
            pltpu.VMEM((2, BS, SHARE), bf16),
            dma((18,)),
            dma((2, 6)),
            dma((2, 6)),
            dma((2, 2)),
            dma((2, 2)),
            dma((2, 2)),
            dma((2, 2)),
            dma((2, 2, 4)),
            dma((2, 2, 4)),
            dma((4,)),
            dma((CHUNKS, 4)),
            dma((2,)),
            dma((CHUNKS,)),
            dma((2,)),
            dma((2,)),
        ],
        compiler_params=pltpu.CompilerParams(
            collective_id=0, has_side_effects=True, vmem_limit_bytes=51 * 1024 * 1024
        ),
        cost_estimate=pl.CostEstimate(
            flops=16 * BS * BS * SHARE, bytes_accessed=16 * BS * BS, transcendentals=0
        ),
    )(table, grad, left, right)


def finish_kernel(
    left_stat, right_stat, left_term, right_term, update, keep,
    left_next, right_next, update_out,
    left_new, right_new, sem,
):
    copies = [pltpu.make_async_copy(update, update_out, sem.at[0])]
    copies[0].start()
    for s in range(2):
        factor = keep[s][:1, :1]
        for side, (stat, term, new, out) in enumerate((
            (left_stat, left_term, left_new, left_next),
            (right_stat, right_term, right_new, right_next),
        )):
            for part in range(2):
                rows = pl.ds(part * (BS // 2), BS // 2)
                new[s, rows] = factor * stat[s, rows] + (1.0 - decay_rate) * f32(term[s, rows])
                copy = pltpu.make_async_copy(
                    new.at[s, rows], out.at[s, rows], sem.at[1 + s * 4 + side * 2 + part]
                )
                copy.start()
                copies.append(copy)
    for copy in copies:
        copy.wait()


def finish(left_stat, right_stat, left_term, right_term, update, keep):
    vmem_spec = pl.BlockSpec(memory_space=pltpu.VMEM)
    stat_shape = jax.ShapeDtypeStruct((2, BS, SHARE), jnp.float32)
    return pl.pallas_call(
        finish_kernel,
        name="shampoo_finish",
        out_shape=(stat_shape, stat_shape, jax.ShapeDtypeStruct(update.shape, update.dtype)),
        in_specs=[vmem_spec] * 6,
        out_specs=(pl.BlockSpec(memory_space=pl.ANY),) * 3,
        scratch_shapes=[
            pltpu.VMEM((2, BS, SHARE), jnp.float32),
            pltpu.VMEM((2, BS, SHARE), jnp.float32),
            pltpu.SemaphoreType.DMA((9,)),
        ],
        compiler_params=pltpu.CompilerParams(vmem_limit_bytes=24 * 1024 * 1024),
        cost_estimate=pl.CostEstimate(flops=4 * BS * BS, bytes_accessed=8 * BS * BS, transcendentals=0),
    )(left_stat, right_stat, left_term, right_term, update, keep)


def on_device(partial_grad, owner_table, left_stat, right_stat, left_root, right_root):
    left_term, right_term, update, keep = exchange(
        owner_table.T,
        partial_grad[0],
        left_root[0].reshape(2, NZ, LANES, SHARE),
        right_root[0],
    )

    left_next, right_next, update = finish(
        left_stat[0], right_stat[0], left_term, right_term, update, keep
    )
    return left_next[None], right_next[None], update


def solution(mesh):
    return jax.shard_map(
        on_device,
        mesh=mesh,
        in_specs=(
            P("rep", None, "fsdp", None),
            P(),
            P("fsdp", None, None, "rep"),
            P("fsdp", None, None, "rep"),
            P("fsdp", None, None, "rep"),
            P("fsdp", None, None, "rep"),
        ),
        out_specs=(
            P("fsdp", None, None, "rep"),
            P("fsdp", None, None, "rep"),
            P(None, "fsdp", "rep"),
        ),
        check_vma=False,
    )
```

```python
import jax
import jax.numpy as jnp
from jax import lax
from jax.experimental import pallas as pl
from jax.experimental.pallas import tpu as pltpu
from jax.sharding import PartitionSpec as P

decay_rate = 0.99

NZ = 8
NY = 8
NX = 4
BLOCKS = 64
HALF = BLOCKS // 2
ROWS = 16
LANES = 128
BS = 1024
SHARE = 256
Z_STEPS = (4, 3, 5, 2, 6, 1, 7)
Y_STEPS = (4, 5, 2, 3, 6, 7, 1)
CHUNK_ORDER = (
    (0, 4), (0, 3), (0, 5), (0, 2), (0, 6), (1, 4), (1, 3), (0, 1),
    (0, 7), (1, 5), (1, 2), (1, 6), (1, 1), (1, 7), (0, 0), (1, 0),
)
CHUNKS = len(CHUNK_ORDER)
BACKWARD = (9, 10, 11, 12)


def lanes(index, width):
    return pl.ds(pl.multiple_of(index * width, width), width)


def wait_for(ref, sem):
    pltpu.make_async_copy(ref, ref, sem).wait()


def send(src, dst, send_sem, recv_sem, device):
    pltpu.make_async_remote_copy(
        src_ref=src,
        dst_ref=dst,
        send_sem=send_sem,
        recv_sem=recv_sem,
        device_id=device,
        device_id_type=pl.DeviceIdType.MESH,
    ).start()


def f32(x):
    return x.astype(jnp.float32)


def kernel(
    table_hbm, grad, left, right,
    left_out, right_out, home, positions_out, keep_out,
    table, table_v, positions, keep, gv, relay_p, relay_m, near_p, near_m, far_p, far_m, shares, copied,
    picked, landed, G, L, R, T, U, back, left_term, right_term,
    local_sem, home_sem, share_sem, rs_s, rs_r, z_s, z_r, y_s, y_r, g_s, g_r, l_s, l_r, bz_s, bz_r, by_s, by_r,
):
    f = lax.axis_index("fsdp")
    x = lax.axis_index("rep")
    z = lax.div(f, NY)
    yc = lax.rem(f, NY)
    nxt = lax.rem(x + 1, NX)
    opp = lax.rem(x + 2, NX)
    prv = lax.rem(x + 3, NX)
    to_nxt = (f, nxt)
    to_prv = (f, prv)

    def z_peer(step):
        return lax.rem(z + step, NZ)

    def y_peer(step):
        return lax.rem(yc + step, NY)

    barrier = pltpu.get_barrier_semaphore()
    peers = [(z_peer(d) * NY + yc, x) for d in Z_STEPS]
    peers += [(z * NY + y_peer(d), x) for d in Y_STEPS]
    peers += [to_nxt, to_prv]
    for peer in peers:
        pl.semaphore_signal(barrier, inc=1, device_id=peer, device_id_type=pl.DeviceIdType.MESH)
    loads = []
    for k in range(2 * NX):
        loads.append(
            pltpu.make_async_copy(
                grad.at[:, :, pl.ds(k * LANES, LANES)], gv.at[k], local_sem.at[0]
            )
        )
    left_loads = []
    for s in range(2):
        left_loads.append(
            pltpu.make_async_copy(
                left.at[s], L.at[s, :, :, lanes(x, SHARE)], local_sem.at[1 + s]
            )
        )
    right_load = pltpu.make_async_copy(right, R, local_sem.at[3])
    table_loads = [
        pltpu.make_async_copy(table_hbm, table, local_sem.at[5]),
        pltpu.make_async_copy(table_hbm, table_v, local_sem.at[6]),
    ]
    for copy in loads + table_loads + left_loads + [right_load]:
        copy.start()

    pl.semaphore_wait(barrier, len(peers))

    wait_for(gv, local_sem.at[0])

    def rs_send(src, dst, kind, h, peer):
        send(src, dst, rs_s.at[kind], rs_r.at[h, min(kind, 2)], peer)

    def rs_first(h):
        rs_send(gv.at[opp * 2 + h, pl.ds(0, HALF)], relay_p.at[h], 0, h, to_nxt)
        rs_send(gv.at[opp * 2 + h, pl.ds(HALF, HALF)], relay_m.at[h], 1, h, to_prv)
        rs_send(gv.at[nxt * 2 + h, pl.ds(HALF, HALF)], near_p.at[h], 2, h, to_nxt)
        rs_send(gv.at[prv * 2 + h, pl.ds(0, HALF)], near_m.at[h], 3, h, to_prv)

    def rs_second(h):
        wait_for(relay_p.at[h], rs_r.at[h, 0])
        relay_p[h] = (f32(relay_p[h]) + f32(gv[nxt * 2 + h, pl.ds(0, HALF)])).astype(jnp.bfloat16)
        rs_send(relay_p.at[h], far_p.at[h], 4, h, to_nxt)
        wait_for(relay_m.at[h], rs_r.at[h, 1])
        relay_m[h] = (f32(relay_m[h]) + f32(gv[prv * 2 + h, pl.ds(HALF, HALF)])).astype(jnp.bfloat16)
        rs_send(relay_m.at[h], far_m.at[h], 5, h, to_prv)

    def pick_from(kind):
        def pick(owner, carry):
            for s in range(2):
                block = table[s, owner]
                index = jnp.maximum(block, 0)
                value = copied[index] if kind == 2 else shares[kind, index]
                picked[kind, s, owner] = jnp.where(block >= 0, value, jnp.zeros_like(value))
            return carry

        lax.fori_loop(0, NZ * NY, pick, 0, unroll=8)

    def rs_final(h):
        wait_for(gv.at[pl.ds(0, 2)], rs_r.at[h, 2])
        own = x * 2 + h
        low = f32(gv[own, pl.ds(0, HALF)]) + f32(near_m[h]) + f32(far_p[h])
        shares[h, pl.ds(0, HALF)] = low.astype(jnp.bfloat16)
        high = f32(gv[own, pl.ds(HALF, HALF)]) + f32(near_p[h]) + f32(far_m[h])
        shares[h, pl.ds(HALF, HALF)] = high.astype(jnp.bfloat16)
        pick_from(h)

    def share_send():
        send(shares.at[0], copied, share_sem.at[0], share_sem.at[1], to_nxt)

    def share_pick():
        wait_for(copied, share_sem.at[1])
        pick_from(2)

    def place_of(kind):
        return lanes(prv * 2 if kind == 2 else x * 2 + kind, LANES)

    def z_send(kind, s):
        for d in Z_STEPS:
            zp = z_peer(d)
            send(
                picked.at[kind, s, pl.ds(zp * NY, NY)], landed.at[kind, s, z],
                z_s.at[0], z_r.at[kind, s], (zp * NY + yc, x),
            )
        landed[kind, s, z] = picked[kind, s, pl.ds(z * NY, NY)]

    def y_send(kind, s):
        wait_for(landed.at[kind, s, pl.ds(0, NZ - 1)], z_r.at[kind, s])
        where = place_of(kind)
        for d in Y_STEPS:
            yp = y_peer(d)
            send(
                landed.at[kind, s, :, yp], G.at[s, :, yc, :, where],
                y_s.at[0], y_r.at[kind, s], (z * NY + yp, x),
            )
        G[s, :, yc, :, where] = landed[kind, s, :, yc]

    def g_send(kind, s):
        where = place_of(kind)
        wait_for(G.at[s, :, pl.ds(0, NY - 1), :, where], y_r.at[kind, s])
        mine = G.at[s, :, :, :, where]
        if kind != 0:
            send(mine, mine, g_s.at[0], g_r.at[kind - 1, s, 0], to_nxt)
        if kind != 2:
            send(mine, mine, g_s.at[1], g_r.at[1 - kind, s, 1], to_prv)

    def g_relay_p(s):
        where = lanes(prv * 2 + 1, LANES)
        wait_for(G.at[s, :, :, :, where], g_r.at[0, s, 0])
        part = G.at[s, pl.ds(0, NZ // 2), :, :, where]
        send(part, part, g_s.at[2], g_r.at[0, s, 2], to_nxt)

    def g_relay_m(s):
        where = lanes(nxt * 2 + 1, LANES)
        wait_for(G.at[s, :, :, :, where], g_r.at[0, s, 1])
        part = G.at[s, pl.ds(NZ // 2, NZ // 2), :, :, where]
        send(part, part, g_s.at[3], g_r.at[0, s, 2], to_prv)

    def g_done(s):
        wait_for(G.at[s, :, :, :, lanes(nxt * 2, LANES)], g_r.at[1, s, 1])
        wait_for(G.at[s, :, :, :, lanes(opp * 2, LANES)], g_r.at[1, s, 0])
        wait_for(G.at[s, :, :, :, lanes(opp * 2 + 1, LANES)], g_r.at[0, s, 2])

    def chunk(c):
        s, step = CHUNK_ORDER[c]
        return s, z_peer(step)

    def l_send_p(c):
        s, zc = chunk(c)
        mine = L.at[s, zc, :, lanes(x, SHARE)]
        send(mine, mine, l_s.at[0], l_r.at[c, 0], to_nxt)

    def l_send_m(c):
        s, zc = chunk(c)
        mine = L.at[s, zc, :, lanes(x, SHARE)]
        send(mine, mine, l_s.at[1], l_r.at[c, 1], to_prv)

    def l_send(c):
        l_send_p(c)
        l_send_m(c)

    def l_relay_p(c):
        s, zc = chunk(c)
        wait_for(L.at[s, zc, :, lanes(prv, SHARE)], l_r.at[c, 0])
        if c not in BACKWARD:
            part = L.at[s, zc, pl.ds(0, LANES // 2), lanes(prv, SHARE)]
            send(part, part, l_s.at[2], l_r.at[c, 2], to_nxt)

    def l_relay_m(c):
        s, zc = chunk(c)
        wait_for(L.at[s, zc, :, lanes(nxt, SHARE)], l_r.at[c, 1])
        first = 0 if c in BACKWARD else LANES // 2
        part = L.at[s, zc, pl.ds(first, LANES - first), lanes(nxt, SHARE)]
        send(part, part, l_s.at[3], l_r.at[c, 2], to_prv)

    def l_relay(c):
        l_relay_p(c)
        l_relay_m(c)

    def right_product(s):
        @pl.loop(0, NZ // 2)
        def _(i):
            rows = G[s, pl.ds(i * 2, 2)].reshape(SHARE, BS)
            result = jnp.dot(rows, R[s], preferred_element_type=jnp.float32)
            T[s, pl.ds(pl.multiple_of(i * SHARE, SHARE), SHARE), :] = result.astype(jnp.bfloat16)

    def left_statistic(s):
        mine = G[s, pl.ds(x * 2, 2)].reshape(SHARE, BS)

        @pl.loop(0, NZ // 2)
        def _(i):
            rows = G[s, pl.ds(i * 2, 2)].reshape(SHARE, BS)
            result = lax.dot_general(
                rows, mine, (((1,), (1,)), ((), ())), preferred_element_type=jnp.float32
            )
            left_term[s, pl.ds(pl.multiple_of(i * SHARE, SHARE), SHARE), :] = result.astype(jnp.bfloat16)

        pltpu.make_async_copy(left_term.at[s], left_out.at[s], local_sem.at[4]).start()

    def right_statistic(s):
        @pl.loop(0, NX)
        def _(i):
            columns = G[s, :, :, :, lanes(i, SHARE)].reshape(BS, SHARE)
            mine = G[s, :, :, :, lanes(x, SHARE)].reshape(BS, SHARE)
            result = lax.dot_general(
                columns, mine, (((0,), (0,)), ((), ())), preferred_element_type=jnp.float32
            )
            right_term[s, pl.ds(pl.multiple_of(i * SHARE, SHARE), SHARE), :] = result.astype(jnp.bfloat16)

        pltpu.make_async_copy(right_term.at[s], right_out.at[s], local_sem.at[4]).start()

    def update_chunk(c):
        s, zc = chunk(c)
        wait_for(L.at[s, zc, :, lanes(opp, SHARE)], l_r.at[c, 2])
        result = jnp.dot(L[s, zc], T[s], preferred_element_type=jnp.float32)
        U[s, zc] = result.astype(jnp.bfloat16).reshape(NY, ROWS, SHARE)
        if CHUNK_ORDER[c][1] == 0:
            back[s, z] = U[s, z]
        else:
            send(U.at[s, zc], back.at[s, z], bz_s.at[0], bz_r.at[c], (zc * NY + yc, x))

    def back_send(c):
        s, step = CHUNK_ORDER[c]
        source = lax.rem(z + NZ - step, NZ)
        if step != 0:
            wait_for(back.at[s, source], bz_r.at[c])
        place = s * NZ * NY + yc * NZ + source
        for d in Y_STEPS:
            yp = y_peer(d)
            send(back.at[s, source, yp], home.at[place], by_s.at[0], by_r.at[0], (z * NY + yp, x))
        pltpu.make_async_copy(back.at[s, source, yc], home.at[place], home_sem.at[0]).start()

    def find_positions():
        table_loads[1].wait()
        total = jnp.zeros((1, LANES), jnp.int32)
        owner = lax.broadcasted_iota(jnp.int32, (NZ * NY, LANES), 0)
        block = lax.broadcasted_iota(jnp.int32, (NZ * NY, LANES), 1)
        slot = lax.rem(owner, NY) * NZ + lax.div(owner, NY)
        for s in range(2):
            row = table_v[pl.ds(s, 1), :]
            held = jnp.broadcast_to(row, (LANES, NZ * NY)).T
            hit = jnp.where(held == block, slot + s * NZ * NY, 0)
            total += jnp.sum(hit, axis=0, keepdims=True)
        positions[...] = jnp.minimum(total, 2 * NZ * NY - 1)
        for s in range(2):
            factor = jnp.where(table[s, f] >= 0, decay_rate, 1.0).astype(jnp.float32)
            keep[s] = jnp.full((8, LANES), factor, jnp.float32)
        table_stores[0].start()
        table_stores[1].start()

    table_stores = [
        pltpu.make_async_copy(positions, positions_out, local_sem.at[7]),
        pltpu.make_async_copy(keep, keep_out, local_sem.at[8]),
    ]

    rs_first(0)
    left_loads[0].wait()
    l_send(0)
    rs_second(0)
    rs_first(1)
    l_send(1)
    table_loads[0].wait()
    rs_final(0)
    z_send(0, 0)
    z_send(0, 1)
    rs_second(1)
    l_send(2)
    l_send(3)
    share_send()
    left_loads[1].wait()
    l_send(4)
    l_send(5)
    find_positions()
    l_relay(0)
    l_relay(1)
    rs_final(1)
    z_send(1, 0)
    y_send(0, 0)
    l_relay(2)
    l_relay(3)
    l_relay_m(4)
    l_relay_m(5)
    g_send(0, 0)
    l_send(6)
    l_send(7)
    y_send(0, 1)
    share_pick()
    z_send(2, 0)
    z_send(1, 1)
    z_send(2, 1)
    l_relay_p(4)
    l_relay_p(5)
    y_send(1, 0)
    l_relay(6)
    g_send(1, 0)
    l_send_m(8)
    l_relay(7)
    y_send(2, 0)
    g_send(2, 0)
    g_relay_p(0)
    g_relay_m(0)
    g_send(0, 1)
    y_send(1, 1)
    g_send(1, 1)
    y_send(2, 1)
    right_load.wait()
    g_done(0)
    g_send(2, 1)
    l_send_m(9)
    right_product(0)
    for c in range(0, 5):
        update_chunk(c)
    update_chunk(7)
    g_relay_m(1)
    l_send_m(10)
    g_relay_p(1)
    l_send_p(8)
    l_send_p(9)
    l_send_p(10)
    l_relay_m(8)
    l_send_m(11)
    left_statistic(0)
    l_relay_m(9)
    l_send_m(12)
    right_statistic(0)
    l_relay_m(10)
    l_send_m(13)
    g_done(1)
    right_product(1)
    update_chunk(5)
    update_chunk(6)
    l_relay_p(8)
    l_send_p(11)
    l_relay_m(11)
    l_send_m(14)
    left_statistic(1)
    l_relay_p(9)
    l_send_p(12)
    l_relay_p(10)
    l_send_p(13)
    update_chunk(8)
    update_chunk(9)
    l_relay_m(12)
    l_send_m(15)
    update_chunk(10)
    right_statistic(1)
    back_send(0)
    back_send(2)
    l_relay_p(11)
    l_send_p(14)
    update_chunk(11)
    l_relay_m(13)
    back_send(1)
    back_send(4)
    l_relay_p(12)
    l_send_p(15)
    l_relay_p(13)
    l_relay_m(14)
    back_send(3)
    update_chunk(12)
    l_relay_p(14)
    l_relay_m(15)
    back_send(7)
    l_relay_p(15)
    update_chunk(13)
    back_send(8)
    back_send(5)
    back_send(6)
    update_chunk(14)
    back_send(14)
    update_chunk(15)
    back_send(15)
    for c in range(9, 14):
        back_send(c)

    for k, ref in enumerate((relay_p, relay_m, near_p, near_m, far_p, far_m)):
        wait_for(ref, rs_s.at[k])
    wait_for(shares.at[0], share_sem.at[0])
    wait_for(picked.at[:, :, pl.ds(0, (NZ - 1) * NY)], z_s.at[0])
    wait_for(landed.at[:, :, :, pl.ds(0, NY - 1)], y_s.at[0])
    where = lanes(x, SHARE)
    for k in range(2):
        wait_for(G.at[:, :, :, :, where], g_s.at[k])
        wait_for(G.at[:, pl.ds(0, NZ // 2), :, :, lanes(x * 2, LANES)], g_s.at[2 + k])
        wait_for(L.at[:, :, :, where], l_s.at[k])
    passed = len(BACKWARD) * LANES // 2
    wait_for(L.at[0, :, pl.ds(0, LANES - passed // NZ), where], l_s.at[2])
    wait_for(L.at[:, pl.ds(0, NZ // 2 + len(BACKWARD) // 4), :, where], l_s.at[3])
    wait_for(gv, local_sem.at[4])
    for copy in table_stores:
        copy.wait()
    wait_for(U.at[:, pl.ds(0, NZ - 1)], bz_s.at[0])
    wait_for(home.at[pl.ds(0, 2 * NZ * (NY - 1))], by_r.at[0])
    wait_for(back.at[:, :, pl.ds(0, NY - 1)], by_s.at[0])
    wait_for(home.at[pl.ds(0, CHUNKS)], home_sem.at[0])


def exchange(table, grad, left, right):
    bf16 = jnp.bfloat16
    any_spec = pl.BlockSpec(memory_space=pl.ANY)
    hbm_spec = pl.BlockSpec(memory_space=pltpu.HBM)
    dma = pltpu.SemaphoreType.DMA
    half = (2, HALF, ROWS, LANES)
    return pl.pallas_call(
        kernel,
        name="shampoo_exchange",
        out_shape=(
            jax.ShapeDtypeStruct((2, BS, SHARE), bf16),
            jax.ShapeDtypeStruct((2, BS, SHARE), bf16),
            jax.ShapeDtypeStruct((2 * NZ * NY, ROWS, SHARE), bf16),
            jax.ShapeDtypeStruct((1, LANES), jnp.int32),
            jax.ShapeDtypeStruct((2, 8, LANES), jnp.float32),
        ),
        in_specs=[hbm_spec, hbm_spec, hbm_spec, hbm_spec],
        out_specs=(any_spec,) * 5,
        scratch_shapes=[
            pltpu.SMEM((2, NZ * NY), jnp.int32),
            pltpu.VMEM((2, NZ * NY), jnp.int32),
            pltpu.VMEM((1, LANES), jnp.int32),
            pltpu.VMEM((2, 8, LANES), jnp.float32),
            pltpu.VMEM((2 * NX, BLOCKS, ROWS, LANES), bf16),
            pltpu.VMEM(half, bf16),
            pltpu.VMEM(half, bf16),
            pltpu.VMEM(half, bf16),
            pltpu.VMEM(half, bf16),
            pltpu.VMEM(half, bf16),
            pltpu.VMEM(half, bf16),
            pltpu.VMEM((2, BLOCKS, ROWS, LANES), bf16),
            pltpu.VMEM((BLOCKS, ROWS, LANES), bf16),
            pltpu.VMEM((3, 2, NZ * NY, ROWS, LANES), bf16),
            pltpu.VMEM((3, 2, NZ, NY, ROWS, LANES), bf16),
            pltpu.VMEM((2, NZ, NY, ROWS, BS), bf16),
            pltpu.VMEM((2, NZ, LANES, BS), bf16),
            pltpu.VMEM((2, BS, SHARE), bf16),
            pltpu.VMEM((2, BS, SHARE), bf16),
            pltpu.VMEM((2, NZ, NY, ROWS, SHARE), bf16),
            pltpu.VMEM((2, NZ, NY, ROWS, SHARE), bf16),
            pltpu.VMEM((2, BS, SHARE), bf16),
            pltpu.VMEM((2, BS, SHARE), bf16),
            dma((9,)),
            dma((1,)),
            dma((2,)),
            dma((6,)),
            dma((2, 3)),
            dma((1,)),
            dma((3, 2)),
            dma((1,)),
            dma((3, 2)),
            dma((4,)),
            dma((2, 2, 3)),
            dma((4,)),
            dma((CHUNKS, 3)),
            dma((1,)),
            dma((CHUNKS,)),
            dma((1,)),
            dma((1,)),
        ],
        compiler_params=pltpu.CompilerParams(
            collective_id=0, has_side_effects=True, vmem_limit_bytes=50 * 1024 * 1024
        ),
        cost_estimate=pl.CostEstimate(
            flops=16 * BS * BS * SHARE, bytes_accessed=16 * BS * BS, transcendentals=0
        ),
    )(table, grad, left, right)


def finish_kernel(
    left_stat, right_stat, left_term, right_term, home, positions_in, keep,
    left_next, right_next, update_out,
    left_new, right_new, positions, sem,
):
    load = pltpu.make_async_copy(positions_in, positions, sem.at[0])
    load.start()
    copies = []

    def next_of(s, stat, term, new, out, part):
        rows = pl.ds(part * (BS // 2), BS // 2)
        new[s, rows] = keep[s][:1, :1] * stat[s, rows] + (1.0 - decay_rate) * f32(term[s, rows])
        copy = pltpu.make_async_copy(new.at[s, rows], out.at[s, rows], sem.at[2 + len(copies)])
        copy.start()
        copies.append(copy)

    next_of(0, left_stat, left_term, left_new, left_next, 0)
    next_of(0, left_stat, left_term, left_new, left_next, 1)
    load.wait()

    def place(b, carry):
        pltpu.make_async_copy(home.at[positions[0, b]], update_out.at[b], sem.at[1]).start()
        return carry

    lax.fori_loop(0, BLOCKS, place, 0, unroll=8)
    for part in range(2):
        next_of(0, right_stat, right_term, right_new, right_next, part)
    for part in range(2):
        next_of(1, left_stat, left_term, left_new, left_next, part)
    for part in range(2):
        next_of(1, right_stat, right_term, right_new, right_next, part)
    for copy in copies:
        copy.wait()
    wait_for(update_out, sem.at[1])


def finish(*operands):
    vmem_spec = pl.BlockSpec(memory_space=pltpu.VMEM)
    any_spec = pl.BlockSpec(memory_space=pl.ANY)
    stat_shape = jax.ShapeDtypeStruct((2, BS, SHARE), jnp.float32)
    return pl.pallas_call(
        finish_kernel,
        name="shampoo_finish",
        out_shape=(
            stat_shape, stat_shape, jax.ShapeDtypeStruct((BLOCKS, ROWS, SHARE), jnp.bfloat16)
        ),
        in_specs=[vmem_spec] * 4 + [any_spec] * 2 + [vmem_spec],
        out_specs=(any_spec,) * 3,
        scratch_shapes=[
            pltpu.VMEM((2, BS, SHARE), jnp.float32),
            pltpu.VMEM((2, BS, SHARE), jnp.float32),
            pltpu.SMEM((1, LANES), jnp.int32),
            pltpu.SemaphoreType.DMA((10,)),
        ],
        compiler_params=pltpu.CompilerParams(vmem_limit_bytes=24 * 1024 * 1024),
        cost_estimate=pl.CostEstimate(flops=4 * BS * BS, bytes_accessed=8 * BS * BS, transcendentals=0),
    )(*operands)


def on_device(partial_grad, owner_table, left_stat, right_stat, left_root, right_root):
    left_term, right_term, home, positions, keep = exchange(
        owner_table.T,
        partial_grad[0],
        left_root[0].reshape(2, NZ, LANES, SHARE),
        right_root[0],
    )

    left_next, right_next, update = finish(
        left_stat[0], right_stat[0], left_term, right_term, home, positions, keep
    )
    return left_next[None], right_next[None], update


def solution(mesh):
    return jax.shard_map(
        on_device,
        mesh=mesh,
        in_specs=(
            P("rep", None, "fsdp", None),
            P(),
            P("fsdp", None, None, "rep"),
            P("fsdp", None, None, "rep"),
            P("fsdp", None, None, "rep"),
            P("fsdp", None, None, "rep"),
        ),
        out_specs=(
            P("fsdp", None, None, "rep"),
            P("fsdp", None, None, "rep"),
            P(None, "fsdp", "rep"),
        ),
        check_vma=False,
    )
```

```python
import jax
import jax.numpy as jnp
from jax import lax
from jax.experimental import pallas as pl
from jax.experimental.pallas import tpu as pltpu
from jax.sharding import PartitionSpec as P

decay_rate = 0.99

NZ = 8
NY = 8
NX = 4
BLOCKS = 64
HALF = BLOCKS // 2
ROWS = 16
LANES = 128
BS = 1024
SHARE = 256
Z_STEPS = (4, 3, 5, 2, 6, 1, 7)
Y_STEPS = (4, 5, 2, 3, 6, 7, 1)
CHUNK_ORDER = (
    (0, 4), (0, 3), (0, 5), (0, 2), (0, 6), (1, 4), (1, 3), (0, 1),
    (0, 7), (1, 5), (1, 2), (1, 6), (1, 1), (1, 7), (0, 0), (1, 0),
)
CHUNKS = len(CHUNK_ORDER)
BACKWARD = (9, 10, 11, 12)


def lanes(index, width):
    return pl.ds(pl.multiple_of(index * width, width), width)


def wait_for(ref, sem):
    pltpu.make_async_copy(ref, ref, sem).wait()


def send(src, dst, send_sem, recv_sem, device):
    pltpu.make_async_remote_copy(
        src_ref=src,
        dst_ref=dst,
        send_sem=send_sem,
        recv_sem=recv_sem,
        device_id=device,
        device_id_type=pl.DeviceIdType.MESH,
    ).start()


def f32(x):
    return x.astype(jnp.float32)


def kernel(
    table_hbm, grad, left, right,
    left_out, right_out, home, positions_out, keep_out,
    table, table_v, positions, keep, gv, relay_p, relay_m, near_p, near_m, far_p, far_m, shares, copied,
    picked, landed, G, L, R, T, U, back, left_term, right_term,
    local_sem, home_sem, share_sem, rs_s, rs_r, z_s, z_r, y_s, y_r, g_s, g_r, l_s, l_r, bz_s, bz_r, by_s, by_r,
):
    f = lax.axis_index("fsdp")
    x = lax.axis_index("rep")
    z = lax.div(f, NY)
    yc = lax.rem(f, NY)
    nxt = lax.rem(x + 1, NX)
    opp = lax.rem(x + 2, NX)
    prv = lax.rem(x + 3, NX)
    to_nxt = (f, nxt)
    to_prv = (f, prv)

    def z_peer(step):
        return lax.rem(z + step, NZ)

    def y_peer(step):
        return lax.rem(yc + step, NY)

    barrier = pltpu.get_barrier_semaphore()
    peers = [(z_peer(d) * NY + yc, x) for d in Z_STEPS]
    peers += [(z * NY + y_peer(d), x) for d in Y_STEPS]
    peers += [to_nxt, to_prv]
    for peer in peers:
        pl.semaphore_signal(barrier, inc=1, device_id=peer, device_id_type=pl.DeviceIdType.MESH)
    loads = []
    for k in range(2 * NX):
        loads.append(
            pltpu.make_async_copy(
                grad.at[:, :, pl.ds(k * LANES, LANES)], gv.at[k], local_sem.at[0]
            )
        )
    left_loads = []
    for s in range(2):
        left_loads.append(
            pltpu.make_async_copy(
                left.at[s], L.at[s, :, :, lanes(x, SHARE)], local_sem.at[1 + s]
            )
        )
    right_load = pltpu.make_async_copy(right, R, local_sem.at[3])
    table_loads = [
        pltpu.make_async_copy(table_hbm, table, local_sem.at[5]),
        pltpu.make_async_copy(table_hbm, table_v, local_sem.at[6]),
    ]
    for copy in loads + table_loads + left_loads + [right_load]:
        copy.start()

    pl.semaphore_wait(barrier, len(peers))

    wait_for(gv, local_sem.at[0])

    def rs_send(src, dst, kind, h, peer):
        send(src, dst, rs_s.at[kind], rs_r.at[h, min(kind, 2)], peer)

    def rs_first(h):
        rs_send(gv.at[opp * 2 + h, pl.ds(0, HALF)], relay_p.at[h], 0, h, to_nxt)
        rs_send(gv.at[opp * 2 + h, pl.ds(HALF, HALF)], relay_m.at[h], 1, h, to_prv)
        rs_send(gv.at[nxt * 2 + h, pl.ds(HALF, HALF)], near_p.at[h], 2, h, to_nxt)
        rs_send(gv.at[prv * 2 + h, pl.ds(0, HALF)], near_m.at[h], 3, h, to_prv)

    def rs_second(h):
        wait_for(relay_p.at[h], rs_r.at[h, 0])
        relay_p[h] = (f32(relay_p[h]) + f32(gv[nxt * 2 + h, pl.ds(0, HALF)])).astype(jnp.bfloat16)
        rs_send(relay_p.at[h], far_p.at[h], 4, h, to_nxt)
        wait_for(relay_m.at[h], rs_r.at[h, 1])
        relay_m[h] = (f32(relay_m[h]) + f32(gv[prv * 2 + h, pl.ds(HALF, HALF)])).astype(jnp.bfloat16)
        rs_send(relay_m.at[h], far_m.at[h], 5, h, to_prv)

    def pick_from(kind):
        def pick(owner, carry):
            for s in range(2):
                block = table[s, owner]
                index = jnp.maximum(block, 0)
                value = copied[index] if kind == 2 else shares[kind, index]
                picked[kind, s, owner] = jnp.where(block >= 0, value, jnp.zeros_like(value))
            return carry

        lax.fori_loop(0, NZ * NY, pick, 0, unroll=8)

    def rs_final(h):
        wait_for(gv.at[pl.ds(0, 2)], rs_r.at[h, 2])
        own = x * 2 + h
        low = f32(gv[own, pl.ds(0, HALF)]) + f32(near_m[h]) + f32(far_p[h])
        shares[h, pl.ds(0, HALF)] = low.astype(jnp.bfloat16)
        high = f32(gv[own, pl.ds(HALF, HALF)]) + f32(near_p[h]) + f32(far_m[h])
        shares[h, pl.ds(HALF, HALF)] = high.astype(jnp.bfloat16)
        pick_from(h)

    def share_send():
        send(shares.at[0], copied, share_sem.at[0], share_sem.at[1], to_nxt)

    def share_pick():
        wait_for(copied, share_sem.at[1])
        pick_from(2)

    def place_of(kind):
        return lanes(prv * 2 if kind == 2 else x * 2 + kind, LANES)

    def z_send(kind, s):
        for d in Z_STEPS:
            zp = z_peer(d)
            send(
                picked.at[kind, s, pl.ds(zp * NY, NY)], landed.at[kind, s, z],
                z_s.at[0], z_r.at[kind, s], (zp * NY + yc, x),
            )
        landed[kind, s, z] = picked[kind, s, pl.ds(z * NY, NY)]

    def y_send(kind, s):
        wait_for(landed.at[kind, s, pl.ds(0, NZ - 1)], z_r.at[kind, s])
        where = place_of(kind)
        for d in Y_STEPS:
            yp = y_peer(d)
            send(
                landed.at[kind, s, :, yp], G.at[s, :, yc, :, where],
                y_s.at[0], y_r.at[kind, s], (z * NY + yp, x),
            )
        G[s, :, yc, :, where] = landed[kind, s, :, yc]

    def g_send(kind, s):
        where = place_of(kind)
        wait_for(G.at[s, :, pl.ds(0, NY - 1), :, where], y_r.at[kind, s])
        mine = G.at[s, :, :, :, where]
        if kind != 0:
            send(mine, mine, g_s.at[0], g_r.at[kind - 1, s, 0], to_nxt)
        if kind != 2:
            send(mine, mine, g_s.at[1], g_r.at[1 - kind, s, 1], to_prv)

    def g_relay_p(s):
        where = lanes(prv * 2 + 1, LANES)
        wait_for(G.at[s, :, :, :, where], g_r.at[0, s, 0])
        part = G.at[s, pl.ds(0, NZ // 2), :, :, where]
        send(part, part, g_s.at[2], g_r.at[0, s, 2], to_nxt)

    def g_relay_m(s):
        where = lanes(nxt * 2 + 1, LANES)
        wait_for(G.at[s, :, :, :, where], g_r.at[0, s, 1])
        part = G.at[s, pl.ds(NZ // 2, NZ // 2), :, :, where]
        send(part, part, g_s.at[3], g_r.at[0, s, 2], to_prv)

    def g_done(s):
        wait_for(G.at[s, :, :, :, lanes(nxt * 2, LANES)], g_r.at[1, s, 1])
        wait_for(G.at[s, :, :, :, lanes(opp * 2, LANES)], g_r.at[1, s, 0])
        wait_for(G.at[s, :, :, :, lanes(opp * 2 + 1, LANES)], g_r.at[0, s, 2])

    def chunk(c):
        s, step = CHUNK_ORDER[c]
        return s, z_peer(step)

    def l_send_p(c):
        s, zc = chunk(c)
        mine = L.at[s, zc, :, lanes(x, SHARE)]
        send(mine, mine, l_s.at[0], l_r.at[c, 0], to_nxt)

    def l_send_m(c):
        s, zc = chunk(c)
        mine = L.at[s, zc, :, lanes(x, SHARE)]
        send(mine, mine, l_s.at[1], l_r.at[c, 1], to_prv)

    def l_send(c):
        l_send_p(c)
        l_send_m(c)

    def l_relay_p(c):
        s, zc = chunk(c)
        wait_for(L.at[s, zc, :, lanes(prv, SHARE)], l_r.at[c, 0])
        if c not in BACKWARD:
            part = L.at[s, zc, pl.ds(0, LANES // 2), lanes(prv, SHARE)]
            send(part, part, l_s.at[2], l_r.at[c, 2], to_nxt)

    def l_relay_m(c):
        s, zc = chunk(c)
        wait_for(L.at[s, zc, :, lanes(nxt, SHARE)], l_r.at[c, 1])
        first = 0 if c in BACKWARD else LANES // 2
        part = L.at[s, zc, pl.ds(first, LANES - first), lanes(nxt, SHARE)]
        send(part, part, l_s.at[3], l_r.at[c, 2], to_prv)

    def l_relay(c):
        l_relay_p(c)
        l_relay_m(c)

    def right_product(s):
        @pl.loop(0, NZ // 2)
        def _(i):
            rows = G[s, pl.ds(i * 2, 2)].reshape(SHARE, BS)
            result = jnp.dot(rows, R[s], preferred_element_type=jnp.float32)
            T[s, pl.ds(pl.multiple_of(i * SHARE, SHARE), SHARE), :] = result.astype(jnp.bfloat16)

    def left_statistic(s):
        mine = G[s, pl.ds(x * 2, 2)].reshape(SHARE, BS)

        @pl.loop(0, NZ // 2)
        def _(i):
            rows = G[s, pl.ds(i * 2, 2)].reshape(SHARE, BS)
            result = lax.dot_general(
                rows, mine, (((1,), (1,)), ((), ())), preferred_element_type=jnp.float32
            )
            left_term[s, pl.ds(pl.multiple_of(i * SHARE, SHARE), SHARE), :] = result.astype(jnp.bfloat16)

        pltpu.make_async_copy(left_term.at[s], left_out.at[s], local_sem.at[4]).start()

    def right_statistic(s):
        @pl.loop(0, NX)
        def _(i):
            columns = G[s, :, :, :, lanes(i, SHARE)].reshape(BS, SHARE)
            mine = G[s, :, :, :, lanes(x, SHARE)].reshape(BS, SHARE)
            result = lax.dot_general(
                columns, mine, (((0,), (0,)), ((), ())), preferred_element_type=jnp.float32
            )
            right_term[s, pl.ds(pl.multiple_of(i * SHARE, SHARE), SHARE), :] = result.astype(jnp.bfloat16)

        pltpu.make_async_copy(right_term.at[s], right_out.at[s], local_sem.at[4]).start()

    def update_chunk(c):
        s, zc = chunk(c)
        wait_for(L.at[s, zc, :, lanes(opp, SHARE)], l_r.at[c, 2])
        result = jnp.dot(L[s, zc], T[s], preferred_element_type=jnp.float32)
        U[s, zc] = result.astype(jnp.bfloat16).reshape(NY, ROWS, SHARE)
        if CHUNK_ORDER[c][1] == 0:
            back[s, z] = U[s, z]
        else:
            send(U.at[s, zc], back.at[s, z], bz_s.at[0], bz_r.at[c], (zc * NY + yc, x))

    def back_send(c):
        s, step = CHUNK_ORDER[c]
        source = lax.rem(z + NZ - step, NZ)
        if step != 0:
            wait_for(back.at[s, source], bz_r.at[c])
        place = s * NZ * NY + yc * NZ + source
        for d in Y_STEPS:
            yp = y_peer(d)
            send(back.at[s, source, yp], home.at[place], by_s.at[0], by_r.at[0], (z * NY + yp, x))
        pltpu.make_async_copy(back.at[s, source, yc], home.at[place], home_sem.at[0]).start()

    def find_positions():
        table_loads[1].wait()
        total = jnp.zeros((1, LANES), jnp.int32)
        owner = lax.broadcasted_iota(jnp.int32, (NZ * NY, LANES), 0)
        block = lax.broadcasted_iota(jnp.int32, (NZ * NY, LANES), 1)
        slot = lax.rem(owner, NY) * NZ + lax.div(owner, NY)
        for s in range(2):
            row = table_v[pl.ds(s, 1), :]
            held = jnp.broadcast_to(row, (LANES, NZ * NY)).T
            hit = jnp.where(held == block, slot + s * NZ * NY, 0)
            total += jnp.sum(hit, axis=0, keepdims=True)
        positions[...] = jnp.minimum(total, 2 * NZ * NY - 1)
        for s in range(2):
            factor = jnp.where(table[s, f] >= 0, decay_rate, 1.0).astype(jnp.float32)
            keep[s] = jnp.full((8, LANES), factor, jnp.float32)
        table_stores[0].start()
        table_stores[1].start()

    table_stores = [
        pltpu.make_async_copy(positions, positions_out, local_sem.at[7]),
        pltpu.make_async_copy(keep, keep_out, local_sem.at[8]),
    ]

    rs_first(0)
    left_loads[0].wait()
    l_send(0)
    rs_second(0)
    rs_first(1)
    l_send(1)
    table_loads[0].wait()
    rs_final(0)
    z_send(0, 0)
    z_send(0, 1)
    rs_second(1)
    l_send(2)
    l_send(3)
    share_send()
    left_loads[1].wait()
    l_send(4)
    l_send(5)
    find_positions()
    l_relay(0)
    l_relay(1)
    rs_final(1)
    z_send(1, 0)
    y_send(0, 0)
    l_relay(2)
    l_relay(3)
    l_relay_m(4)
    l_relay_m(5)
    g_send(0, 0)
    l_send(6)
    l_send(7)
    y_send(0, 1)
    share_pick()
    z_send(2, 0)
    z_send(1, 1)
    z_send(2, 1)
    l_relay_p(4)
    l_relay_p(5)
    l_send(8)
    y_send(1, 0)
    l_relay(6)
    g_send(1, 0)
    l_relay(7)
    y_send(2, 0)
    g_send(2, 0)
    g_relay_p(0)
    g_relay_m(0)
    g_send(0, 1)
    y_send(1, 1)
    g_send(1, 1)
    y_send(2, 1)
    right_load.wait()
    g_done(0)
    g_send(2, 1)
    l_send_m(9)
    right_product(0)
    for c in range(0, 5):
        update_chunk(c)
    update_chunk(7)
    g_relay_m(1)
    l_send_m(10)
    g_relay_p(1)
    l_send_p(9)
    l_send_p(10)
    l_send_p(11)
    l_relay_m(8)
    l_send_m(11)
    left_statistic(0)
    l_relay_m(9)
    l_send_m(12)
    right_statistic(0)
    l_relay_m(10)
    l_send_m(13)
    g_done(1)
    right_product(1)
    update_chunk(5)
    update_chunk(6)
    back_send(0)
    back_send(2)
    l_relay_p(8)
    l_send_p(12)
    l_relay_m(11)
    l_send_m(14)
    left_statistic(1)
    l_relay_p(9)
    l_send_p(13)
    l_relay_p(10)
    l_send_p(14)
    update_chunk(8)
    update_chunk(9)
    l_relay_m(12)
    l_send_m(15)
    l_send_p(15)
    update_chunk(10)
    back_send(1)
    back_send(4)
    right_statistic(1)
    l_relay_p(11)
    update_chunk(11)
    l_relay_m(13)
    l_relay_p(12)
    l_relay_p(13)
    l_relay_m(14)
    back_send(3)
    update_chunk(12)
    l_relay_p(14)
    l_relay_m(15)
    back_send(7)
    l_relay_p(15)
    update_chunk(13)
    back_send(8)
    back_send(5)
    back_send(6)
    back_send(9)
    update_chunk(14)
    back_send(14)
    back_send(10)
    update_chunk(15)
    back_send(15)
    back_send(11)
    back_send(12)
    back_send(13)

    for k, ref in enumerate((relay_p, relay_m, near_p, near_m, far_p, far_m)):
        wait_for(ref, rs_s.at[k])
    wait_for(shares.at[0], share_sem.at[0])
    wait_for(picked.at[:, :, pl.ds(0, (NZ - 1) * NY)], z_s.at[0])
    wait_for(landed.at[:, :, :, pl.ds(0, NY - 1)], y_s.at[0])
    where = lanes(x, SHARE)
    for k in range(2):
        wait_for(G.at[:, :, :, :, where], g_s.at[k])
        wait_for(G.at[:, pl.ds(0, NZ // 2), :, :, lanes(x * 2, LANES)], g_s.at[2 + k])
        wait_for(L.at[:, :, :, where], l_s.at[k])
    passed = len(BACKWARD) * LANES // 2
    wait_for(L.at[0, :, pl.ds(0, LANES - passed // NZ), where], l_s.at[2])
    wait_for(L.at[:, pl.ds(0, NZ // 2 + len(BACKWARD) // 4), :, where], l_s.at[3])
    wait_for(gv, local_sem.at[4])
    for copy in table_stores:
        copy.wait()
    wait_for(U.at[:, pl.ds(0, NZ - 1)], bz_s.at[0])
    wait_for(home.at[pl.ds(0, 2 * NZ * (NY - 1))], by_r.at[0])
    wait_for(back.at[:, :, pl.ds(0, NY - 1)], by_s.at[0])
    wait_for(home.at[pl.ds(0, CHUNKS)], home_sem.at[0])


def exchange(table, grad, left, right):
    bf16 = jnp.bfloat16
    any_spec = pl.BlockSpec(memory_space=pl.ANY)
    hbm_spec = pl.BlockSpec(memory_space=pltpu.HBM)
    dma = pltpu.SemaphoreType.DMA
    half = (2, HALF, ROWS, LANES)
    return pl.pallas_call(
        kernel,
        name="shampoo_exchange",
        out_shape=(
            jax.ShapeDtypeStruct((2, BS, SHARE), bf16),
            jax.ShapeDtypeStruct((2, BS, SHARE), bf16),
            jax.ShapeDtypeStruct((2 * NZ * NY, ROWS, SHARE), bf16),
            jax.ShapeDtypeStruct((1, LANES), jnp.int32),
            jax.ShapeDtypeStruct((2, 8, LANES), jnp.float32),
        ),
        in_specs=[hbm_spec, hbm_spec, hbm_spec, hbm_spec],
        out_specs=(any_spec,) * 5,
        scratch_shapes=[
            pltpu.SMEM((2, NZ * NY), jnp.int32),
            pltpu.VMEM((2, NZ * NY), jnp.int32),
            pltpu.VMEM((1, LANES), jnp.int32),
            pltpu.VMEM((2, 8, LANES), jnp.float32),
            pltpu.VMEM((2 * NX, BLOCKS, ROWS, LANES), bf16),
            pltpu.VMEM(half, bf16),
            pltpu.VMEM(half, bf16),
            pltpu.VMEM(half, bf16),
            pltpu.VMEM(half, bf16),
            pltpu.VMEM(half, bf16),
            pltpu.VMEM(half, bf16),
            pltpu.VMEM((2, BLOCKS, ROWS, LANES), bf16),
            pltpu.VMEM((BLOCKS, ROWS, LANES), bf16),
            pltpu.VMEM((3, 2, NZ * NY, ROWS, LANES), bf16),
            pltpu.VMEM((3, 2, NZ, NY, ROWS, LANES), bf16),
            pltpu.VMEM((2, NZ, NY, ROWS, BS), bf16),
            pltpu.VMEM((2, NZ, LANES, BS), bf16),
            pltpu.VMEM((2, BS, SHARE), bf16),
            pltpu.VMEM((2, BS, SHARE), bf16),
            pltpu.VMEM((2, NZ, NY, ROWS, SHARE), bf16),
            pltpu.VMEM((2, NZ, NY, ROWS, SHARE), bf16),
            pltpu.VMEM((2, BS, SHARE), bf16),
            pltpu.VMEM((2, BS, SHARE), bf16),
            dma((9,)),
            dma((1,)),
            dma((2,)),
            dma((6,)),
            dma((2, 3)),
            dma((1,)),
            dma((3, 2)),
            dma((1,)),
            dma((3, 2)),
            dma((4,)),
            dma((2, 2, 3)),
            dma((4,)),
            dma((CHUNKS, 3)),
            dma((1,)),
            dma((CHUNKS,)),
            dma((1,)),
            dma((1,)),
        ],
        compiler_params=pltpu.CompilerParams(
            collective_id=0, has_side_effects=True, vmem_limit_bytes=50 * 1024 * 1024
        ),
        cost_estimate=pl.CostEstimate(
            flops=16 * BS * BS * SHARE, bytes_accessed=16 * BS * BS, transcendentals=0
        ),
    )(table, grad, left, right)


def finish_kernel(
    left_stat, right_stat, left_term, right_term, home, positions_in, keep,
    left_next, right_next, update_out,
    left_new, right_new, positions, sem,
):
    load = pltpu.make_async_copy(positions_in, positions, sem.at[0])
    load.start()
    copies = []

    def next_of(s, stat, term, new, out, part):
        rows = pl.ds(part * (BS // 2), BS // 2)
        new[s, rows] = keep[s][:1, :1] * stat[s, rows] + (1.0 - decay_rate) * f32(term[s, rows])
        copy = pltpu.make_async_copy(new.at[s, rows], out.at[s, rows], sem.at[2 + len(copies)])
        copy.start()
        copies.append(copy)

    sides = (
        (left_stat, left_term, left_new, left_next),
        (right_stat, right_term, right_new, right_next),
    )
    parts = [(s, side, part) for s in range(2) for side in sides for part in range(2)]
    placed = 0
    for k, (s, side, part) in enumerate(parts):
        next_of(s, *side, part)
        if k == 1:
            load.wait()
        if k >= 1:
            upto = BLOCKS * k // (len(parts) - 1)
            for b in range(placed, upto):
                pltpu.make_async_copy(home.at[positions[0, b]], update_out.at[b], sem.at[1]).start()
            placed = upto
    for copy in copies:
        copy.wait()
    wait_for(update_out, sem.at[1])


def finish(*operands):
    vmem_spec = pl.BlockSpec(memory_space=pltpu.VMEM)
    any_spec = pl.BlockSpec(memory_space=pl.ANY)
    stat_shape = jax.ShapeDtypeStruct((2, BS, SHARE), jnp.float32)
    return pl.pallas_call(
        finish_kernel,
        name="shampoo_finish",
        out_shape=(
            stat_shape, stat_shape, jax.ShapeDtypeStruct((BLOCKS, ROWS, SHARE), jnp.bfloat16)
        ),
        in_specs=[vmem_spec] * 4 + [any_spec] * 2 + [vmem_spec],
        out_specs=(any_spec,) * 3,
        scratch_shapes=[
            pltpu.VMEM((2, BS, SHARE), jnp.float32),
            pltpu.VMEM((2, BS, SHARE), jnp.float32),
            pltpu.SMEM((1, LANES), jnp.int32),
            pltpu.SemaphoreType.DMA((10,)),
        ],
        compiler_params=pltpu.CompilerParams(vmem_limit_bytes=24 * 1024 * 1024),
        cost_estimate=pl.CostEstimate(flops=4 * BS * BS, bytes_accessed=8 * BS * BS, transcendentals=0),
    )(*operands)


def on_device(partial_grad, owner_table, left_stat, right_stat, left_root, right_root):
    left_term, right_term, home, positions, keep = exchange(
        owner_table.T,
        partial_grad[0],
        left_root[0].reshape(2, NZ, LANES, SHARE),
        right_root[0],
    )

    left_next, right_next, update = finish(
        left_stat[0], right_stat[0], left_term, right_term, home, positions, keep
    )
    return left_next[None], right_next[None], update


def solution(mesh):
    return jax.shard_map(
        on_device,
        mesh=mesh,
        in_specs=(
            P("rep", None, "fsdp", None),
            P(),
            P("fsdp", None, None, "rep"),
            P("fsdp", None, None, "rep"),
            P("fsdp", None, None, "rep"),
            P("fsdp", None, None, "rep"),
        ),
        out_specs=(
            P("fsdp", None, None, "rep"),
            P("fsdp", None, None, "rep"),
            P(None, "fsdp", "rep"),
        ),
        check_vma=False,
    )
```

```python
import jax
import jax.numpy as jnp
from jax import lax
from jax.experimental import pallas as pl
from jax.experimental.pallas import tpu as pltpu
from jax.sharding import PartitionSpec as P

decay_rate = 0.99

NZ = 8
NY = 8
NX = 4
BLOCKS = 64
HALF = BLOCKS // 2
ROWS = 16
LANES = 128
BS = 1024
SHARE = 256
Z_STEPS = (4, 3, 5, 2, 6, 1, 7)
Y_STEPS = (4, 5, 2, 3, 6, 7, 1)
CHUNK_ORDER = (
    (0, 4), (0, 3), (0, 5), (0, 2), (0, 6), (1, 4), (1, 3), (0, 1),
    (0, 7), (1, 5), (1, 2), (1, 6), (1, 1), (1, 7), (0, 0), (1, 0),
)
CHUNKS = len(CHUNK_ORDER)
BACKWARD = (9, 10, 11, 12)
TOGETHER = (0, 1, 2, 3, 4, 7)
LATER = tuple(c for c in range(CHUNKS) if c not in TOGETHER)


def lanes(index, width):
    return pl.ds(pl.multiple_of(index * width, width), width)


def wait_for(ref, sem):
    pltpu.make_async_copy(ref, ref, sem).wait()


def send(src, dst, send_sem, recv_sem, device):
    pltpu.make_async_remote_copy(
        src_ref=src,
        dst_ref=dst,
        send_sem=send_sem,
        recv_sem=recv_sem,
        device_id=device,
        device_id_type=pl.DeviceIdType.MESH,
    ).start()


def f32(x):
    return x.astype(jnp.float32)


def kernel(
    table_hbm, grad, left, right,
    left_out, right_out, home, positions_out, keep_out,
    table, table_v, positions, keep, gv, relay_p, relay_m, near_p, near_m, far_p, far_m, shares, copied,
    picked, landed, G, L, R, T, U, back, left_term, right_term,
    local_sem, home_sem, passed_sem, share_sem, rs_s, rs_r, z_s, z_r, y_s, y_r, g_s, g_r, l_s, l_r, bz_s, bz_r, by_s, by_r,
):
    f = lax.axis_index("fsdp")
    x = lax.axis_index("rep")
    z = lax.div(f, NY)
    yc = lax.rem(f, NY)
    nxt = lax.rem(x + 1, NX)
    opp = lax.rem(x + 2, NX)
    prv = lax.rem(x + 3, NX)
    to_nxt = (f, nxt)
    to_prv = (f, prv)

    def z_peer(step):
        return lax.rem(z + step, NZ)

    def y_peer(step):
        return lax.rem(yc + step, NY)

    barrier = pltpu.get_barrier_semaphore()
    peers = [(z_peer(d) * NY + yc, x) for d in Z_STEPS]
    peers += [(z * NY + y_peer(d), x) for d in Y_STEPS]
    peers += [to_nxt, to_prv]
    for peer in peers:
        pl.semaphore_signal(barrier, inc=1, device_id=peer, device_id_type=pl.DeviceIdType.MESH)
    loads = []
    for k in range(2 * NX):
        loads.append(
            pltpu.make_async_copy(
                grad.at[:, :, pl.ds(k * LANES, LANES)], gv.at[k], local_sem.at[0]
            )
        )
    left_loads = []
    for s in range(2):
        left_loads.append(
            pltpu.make_async_copy(
                left.at[s], L.at[s, :, :, lanes(x, SHARE)], local_sem.at[1 + s]
            )
        )
    right_load = pltpu.make_async_copy(right, R, local_sem.at[3])
    table_loads = [
        pltpu.make_async_copy(table_hbm, table, local_sem.at[5]),
        pltpu.make_async_copy(table_hbm, table_v, local_sem.at[6]),
    ]
    for copy in loads + table_loads + left_loads + [right_load]:
        copy.start()

    pl.semaphore_wait(barrier, len(peers))

    wait_for(gv, local_sem.at[0])

    def rs_send(src, dst, kind, h, peer):
        send(src, dst, rs_s.at[kind], rs_r.at[h, min(kind, 2)], peer)

    def rs_first(h):
        rs_send(gv.at[opp * 2 + h, pl.ds(0, HALF)], relay_p.at[h], 0, h, to_nxt)
        rs_send(gv.at[opp * 2 + h, pl.ds(HALF, HALF)], relay_m.at[h], 1, h, to_prv)
        rs_send(gv.at[nxt * 2 + h, pl.ds(HALF, HALF)], near_p.at[h], 2, h, to_nxt)
        rs_send(gv.at[prv * 2 + h, pl.ds(0, HALF)], near_m.at[h], 3, h, to_prv)

    def rs_second(h):
        wait_for(relay_p.at[h], rs_r.at[h, 0])
        relay_p[h] = (f32(relay_p[h]) + f32(gv[nxt * 2 + h, pl.ds(0, HALF)])).astype(jnp.bfloat16)
        rs_send(relay_p.at[h], far_p.at[h], 4, h, to_nxt)
        wait_for(relay_m.at[h], rs_r.at[h, 1])
        relay_m[h] = (f32(relay_m[h]) + f32(gv[prv * 2 + h, pl.ds(HALF, HALF)])).astype(jnp.bfloat16)
        rs_send(relay_m.at[h], far_m.at[h], 5, h, to_prv)

    def pick_from(kind):
        def pick(owner, carry):
            for s in range(2):
                block = table[s, owner]
                index = jnp.maximum(block, 0)
                value = copied[index] if kind == 2 else shares[kind, index]
                picked[kind, s, owner] = jnp.where(block >= 0, value, jnp.zeros_like(value))
            return carry

        lax.fori_loop(0, NZ * NY, pick, 0, unroll=8)

    def rs_final(h):
        wait_for(gv.at[pl.ds(0, 2)], rs_r.at[h, 2])
        own = x * 2 + h
        low = f32(gv[own, pl.ds(0, HALF)]) + f32(near_m[h]) + f32(far_p[h])
        shares[h, pl.ds(0, HALF)] = low.astype(jnp.bfloat16)
        high = f32(gv[own, pl.ds(HALF, HALF)]) + f32(near_p[h]) + f32(far_m[h])
        shares[h, pl.ds(HALF, HALF)] = high.astype(jnp.bfloat16)
        pick_from(h)

    def share_send():
        send(shares.at[0], copied, share_sem.at[0], share_sem.at[1], to_nxt)

    def share_pick():
        wait_for(copied, share_sem.at[1])
        pick_from(2)

    def place_of(kind):
        return lanes(prv * 2 if kind == 2 else x * 2 + kind, LANES)

    def z_send(kind, s):
        for d in Z_STEPS:
            zp = z_peer(d)
            send(
                picked.at[kind, s, pl.ds(zp * NY, NY)], landed.at[kind, s, z],
                z_s.at[0], z_r.at[kind, s], (zp * NY + yc, x),
            )
        landed[kind, s, z] = picked[kind, s, pl.ds(z * NY, NY)]

    def y_send(kind, s):
        wait_for(landed.at[kind, s, pl.ds(0, NZ - 1)], z_r.at[kind, s])
        where = place_of(kind)
        for d in Y_STEPS:
            yp = y_peer(d)
            send(
                landed.at[kind, s, :, yp], G.at[s, :, yc, :, where],
                y_s.at[0], y_r.at[kind, s], (z * NY + yp, x),
            )
        G[s, :, yc, :, where] = landed[kind, s, :, yc]

    def g_send(kind, s):
        where = place_of(kind)
        wait_for(G.at[s, :, pl.ds(0, NY - 1), :, where], y_r.at[kind, s])
        mine = G.at[s, :, :, :, where]
        if kind != 0:
            send(mine, mine, g_s.at[0], g_r.at[kind - 1, s, 0], to_nxt)
        if kind != 2:
            send(mine, mine, g_s.at[1], g_r.at[1 - kind, s, 1], to_prv)

    def g_relay_p(s):
        where = lanes(prv * 2 + 1, LANES)
        wait_for(G.at[s, :, :, :, where], g_r.at[0, s, 0])
        part = G.at[s, pl.ds(0, NZ // 2), :, :, where]
        send(part, part, g_s.at[2], g_r.at[0, s, 2], to_nxt)

    def g_relay_m(s):
        where = lanes(nxt * 2 + 1, LANES)
        wait_for(G.at[s, :, :, :, where], g_r.at[0, s, 1])
        part = G.at[s, pl.ds(NZ // 2, NZ // 2), :, :, where]
        send(part, part, g_s.at[3], g_r.at[0, s, 2], to_prv)

    def g_done(s):
        wait_for(G.at[s, :, :, :, lanes(nxt * 2, LANES)], g_r.at[1, s, 1])
        wait_for(G.at[s, :, :, :, lanes(opp * 2, LANES)], g_r.at[1, s, 0])
        wait_for(G.at[s, :, :, :, lanes(opp * 2 + 1, LANES)], g_r.at[0, s, 2])

    def chunk(c):
        s, step = CHUNK_ORDER[c]
        return s, z_peer(step)

    def l_send_p(c):
        s, zc = chunk(c)
        mine = L.at[s, zc, :, lanes(x, SHARE)]
        send(mine, mine, l_s.at[0], l_r.at[c, 0], to_nxt)

    def l_send_m(c):
        s, zc = chunk(c)
        mine = L.at[s, zc, :, lanes(x, SHARE)]
        send(mine, mine, l_s.at[1], l_r.at[c, 1], to_prv)

    def l_send(c):
        l_send_p(c)
        l_send_m(c)

    def relayed(c):
        return passed_sem.at[0 if c in TOGETHER else 1 + LATER.index(c)]

    def l_relay_p(c):
        s, zc = chunk(c)
        wait_for(L.at[s, zc, :, lanes(prv, SHARE)], l_r.at[c, 0])
        if c not in BACKWARD:
            part = L.at[s, zc, pl.ds(0, LANES // 2), lanes(prv, SHARE)]
            send(part, part, l_s.at[2], relayed(c), to_nxt)

    def l_relay_m(c):
        s, zc = chunk(c)
        wait_for(L.at[s, zc, :, lanes(nxt, SHARE)], l_r.at[c, 1])
        first = 0 if c in BACKWARD else LANES // 2
        part = L.at[s, zc, pl.ds(first, LANES - first), lanes(nxt, SHARE)]
        send(part, part, l_s.at[3], relayed(c), to_prv)

    def l_relay(c):
        l_relay_p(c)
        l_relay_m(c)

    def right_product(s):
        @pl.loop(0, NZ // 2)
        def _(i):
            rows = G[s, pl.ds(i * 2, 2)].reshape(SHARE, BS)
            result = jnp.dot(rows, R[s], preferred_element_type=jnp.float32)
            T[s, pl.ds(pl.multiple_of(i * SHARE, SHARE), SHARE), :] = result.astype(jnp.bfloat16)

    def left_statistic(s):
        mine = G[s, pl.ds(x * 2, 2)].reshape(SHARE, BS)

        @pl.loop(0, NZ // 2)
        def _(i):
            rows = G[s, pl.ds(i * 2, 2)].reshape(SHARE, BS)
            result = lax.dot_general(
                rows, mine, (((1,), (1,)), ((), ())), preferred_element_type=jnp.float32
            )
            left_term[s, pl.ds(pl.multiple_of(i * SHARE, SHARE), SHARE), :] = result.astype(jnp.bfloat16)

        pltpu.make_async_copy(left_term.at[s], left_out.at[s], local_sem.at[4]).start()

    def right_statistic(s):
        @pl.loop(0, NX)
        def _(i):
            columns = G[s, :, :, :, lanes(i, SHARE)].reshape(BS, SHARE)
            mine = G[s, :, :, :, lanes(x, SHARE)].reshape(BS, SHARE)
            result = lax.dot_general(
                columns, mine, (((0,), (0,)), ((), ())), preferred_element_type=jnp.float32
            )
            right_term[s, pl.ds(pl.multiple_of(i * SHARE, SHARE), SHARE), :] = result.astype(jnp.bfloat16)

        pltpu.make_async_copy(right_term.at[s], right_out.at[s], local_sem.at[4]).start()

    def update_chunk(c):
        s, zc = chunk(c)
        if c not in TOGETHER:
            wait_for(L.at[s, zc, :, lanes(opp, SHARE)], relayed(c))
        result = jnp.dot(L[s, zc], T[s], preferred_element_type=jnp.float32)
        U[s, zc] = result.astype(jnp.bfloat16).reshape(NY, ROWS, SHARE)
        if CHUNK_ORDER[c][1] == 0:
            back[s, z] = U[s, z]
        else:
            send(U.at[s, zc], back.at[s, z], bz_s.at[0], bz_r.at[c], (zc * NY + yc, x))

    def back_send(c):
        s, step = CHUNK_ORDER[c]
        source = lax.rem(z + NZ - step, NZ)
        if step != 0:
            wait_for(back.at[s, source], bz_r.at[c])
        place = s * NZ * NY + yc * NZ + source
        for d in Y_STEPS:
            yp = y_peer(d)
            send(back.at[s, source, yp], home.at[place], by_s.at[0], by_r.at[0], (z * NY + yp, x))
        pltpu.make_async_copy(back.at[s, source, yc], home.at[place], home_sem.at[0]).start()

    def find_positions():
        table_loads[1].wait()
        total = jnp.zeros((1, LANES), jnp.int32)
        owner = lax.broadcasted_iota(jnp.int32, (NZ * NY, LANES), 0)
        block = lax.broadcasted_iota(jnp.int32, (NZ * NY, LANES), 1)
        slot = lax.rem(owner, NY) * NZ + lax.div(owner, NY)
        for s in range(2):
            row = table_v[pl.ds(s, 1), :]
            held = jnp.broadcast_to(row, (LANES, NZ * NY)).T
            hit = jnp.where(held == block, slot + s * NZ * NY, 0)
            total += jnp.sum(hit, axis=0, keepdims=True)
        positions[...] = jnp.minimum(total, 2 * NZ * NY - 1)
        for s in range(2):
            factor = jnp.where(table[s, f] >= 0, decay_rate, 1.0).astype(jnp.float32)
            keep[s] = jnp.full((8, LANES), factor, jnp.float32)
        table_stores[0].start()
        table_stores[1].start()

    table_stores = [
        pltpu.make_async_copy(positions, positions_out, local_sem.at[7]),
        pltpu.make_async_copy(keep, keep_out, local_sem.at[8]),
    ]

    rs_first(0)
    left_loads[0].wait()
    l_send(0)
    rs_second(0)
    rs_first(1)
    l_send(1)
    table_loads[0].wait()
    rs_final(0)
    z_send(0, 0)
    z_send(0, 1)
    rs_second(1)
    l_send(2)
    l_send(3)
    share_send()
    left_loads[1].wait()
    l_send(4)
    l_send(5)
    find_positions()
    l_relay(0)
    l_relay(1)
    rs_final(1)
    z_send(1, 0)
    y_send(0, 0)
    l_relay(2)
    l_relay(3)
    l_relay_m(4)
    l_relay_m(5)
    g_send(0, 0)
    l_send(6)
    l_send(7)
    y_send(0, 1)
    share_pick()
    z_send(2, 0)
    z_send(1, 1)
    z_send(2, 1)
    l_relay_p(4)
    l_relay_p(5)
    l_send(8)
    y_send(1, 0)
    l_relay(6)
    g_send(1, 0)
    l_relay(7)
    y_send(2, 0)
    g_send(2, 0)
    g_relay_m(0)
    g_relay_p(0)
    g_send(0, 1)
    y_send(1, 1)
    g_send(1, 1)
    y_send(2, 1)
    right_load.wait()
    g_done(0)
    g_send(2, 1)
    l_send_m(9)
    right_product(0)
    wait_for(L.at[0, pl.ds(0, len(TOGETHER)), :, lanes(opp, SHARE)], passed_sem.at[0])
    for c in range(0, 5):
        update_chunk(c)
    update_chunk(7)
    g_relay_m(1)
    l_send_m(10)
    g_relay_p(1)
    l_send_p(9)
    l_send_p(10)
    l_send_p(11)
    l_relay_m(8)
    l_send_m(11)
    left_statistic(0)
    l_relay_m(9)
    l_send_m(12)
    right_statistic(0)
    l_relay_m(10)
    l_send_m(13)
    g_done(1)
    right_product(1)
    update_chunk(5)
    update_chunk(6)
    back_send(0)
    back_send(2)
    l_relay_p(8)
    l_send_p(12)
    l_relay_m(11)
    l_send_m(14)
    left_statistic(1)
    l_relay_p(9)
    l_send_p(13)
    l_relay_p(10)
    l_send_p(14)
    update_chunk(8)
    update_chunk(9)
    l_relay_m(12)
    l_send_m(15)
    l_send_p(15)
    update_chunk(10)
    back_send(1)
    back_send(4)
    right_statistic(1)
    l_relay_p(11)
    update_chunk(11)
    l_relay_m(13)
    l_relay_p(12)
    l_relay_p(13)
    l_relay_m(14)
    back_send(3)
    update_chunk(12)
    l_relay_p(14)
    l_relay_m(15)
    l_relay_p(15)
    back_send(7)
    back_send(8)
    back_send(5)
    update_chunk(13)
    back_send(6)
    back_send(9)
    back_send(10)
    update_chunk(14)
    back_send(14)
    update_chunk(15)
    back_send(15)
    back_send(11)
    back_send(12)
    back_send(13)

    for k, ref in enumerate((relay_p, relay_m, near_p, near_m, far_p, far_m)):
        wait_for(ref, rs_s.at[k])
    wait_for(shares.at[0], share_sem.at[0])
    wait_for(picked.at[:, :, pl.ds(0, (NZ - 1) * NY)], z_s.at[0])
    wait_for(landed.at[:, :, :, pl.ds(0, NY - 1)], y_s.at[0])
    where = lanes(x, SHARE)
    for k in range(2):
        wait_for(G.at[:, :, :, :, where], g_s.at[k])
        wait_for(G.at[:, pl.ds(0, NZ // 2), :, :, lanes(x * 2, LANES)], g_s.at[2 + k])
        wait_for(L.at[:, :, :, where], l_s.at[k])
    passed = len(BACKWARD) * LANES // 2
    wait_for(L.at[0, :, pl.ds(0, LANES - passed // NZ), where], l_s.at[2])
    wait_for(L.at[:, pl.ds(0, NZ // 2 + len(BACKWARD) // 4), :, where], l_s.at[3])
    wait_for(gv, local_sem.at[4])
    for copy in table_stores:
        copy.wait()
    wait_for(U.at[:, pl.ds(0, NZ - 1)], bz_s.at[0])
    wait_for(home.at[pl.ds(0, 2 * NZ * (NY - 1))], by_r.at[0])
    wait_for(back.at[:, :, pl.ds(0, NY - 1)], by_s.at[0])
    wait_for(home.at[pl.ds(0, CHUNKS)], home_sem.at[0])


def exchange(table, grad, left, right):
    bf16 = jnp.bfloat16
    any_spec = pl.BlockSpec(memory_space=pl.ANY)
    hbm_spec = pl.BlockSpec(memory_space=pltpu.HBM)
    dma = pltpu.SemaphoreType.DMA
    half = (2, HALF, ROWS, LANES)
    return pl.pallas_call(
        kernel,
        name="shampoo_exchange",
        out_shape=(
            jax.ShapeDtypeStruct((2, BS, SHARE), bf16),
            jax.ShapeDtypeStruct((2, BS, SHARE), bf16),
            jax.ShapeDtypeStruct((2 * NZ * NY, ROWS, SHARE), bf16),
            jax.ShapeDtypeStruct((1, LANES), jnp.int32),
            jax.ShapeDtypeStruct((2, 8, LANES), jnp.float32),
        ),
        in_specs=[hbm_spec, hbm_spec, hbm_spec, hbm_spec],
        out_specs=(any_spec,) * 5,
        scratch_shapes=[
            pltpu.SMEM((2, NZ * NY), jnp.int32),
            pltpu.VMEM((2, NZ * NY), jnp.int32),
            pltpu.VMEM((1, LANES), jnp.int32),
            pltpu.VMEM((2, 8, LANES), jnp.float32),
            pltpu.VMEM((2 * NX, BLOCKS, ROWS, LANES), bf16),
            pltpu.VMEM(half, bf16),
            pltpu.VMEM(half, bf16),
            pltpu.VMEM(half, bf16),
            pltpu.VMEM(half, bf16),
            pltpu.VMEM(half, bf16),
            pltpu.VMEM(half, bf16),
            pltpu.VMEM((2, BLOCKS, ROWS, LANES), bf16),
            pltpu.VMEM((BLOCKS, ROWS, LANES), bf16),
            pltpu.VMEM((3, 2, NZ * NY, ROWS, LANES), bf16),
            pltpu.VMEM((3, 2, NZ, NY, ROWS, LANES), bf16),
            pltpu.VMEM((2, NZ, NY, ROWS, BS), bf16),
            pltpu.VMEM((2, NZ, LANES, BS), bf16),
            pltpu.VMEM((2, BS, SHARE), bf16),
            pltpu.VMEM((2, BS, SHARE), bf16),
            pltpu.VMEM((2, NZ, NY, ROWS, SHARE), bf16),
            pltpu.VMEM((2, NZ, NY, ROWS, SHARE), bf16),
            pltpu.VMEM((2, BS, SHARE), bf16),
            pltpu.VMEM((2, BS, SHARE), bf16),
            dma((9,)),
            dma((1,)),
            dma((1 + len(LATER),)),
            dma((2,)),
            dma((6,)),
            dma((2, 3)),
            dma((1,)),
            dma((3, 2)),
            dma((1,)),
            dma((3, 2)),
            dma((4,)),
            dma((2, 2, 3)),
            dma((4,)),
            dma((CHUNKS, 2)),
            dma((1,)),
            dma((CHUNKS,)),
            dma((1,)),
            dma((1,)),
        ],
        compiler_params=pltpu.CompilerParams(
            collective_id=0, has_side_effects=True, vmem_limit_bytes=50 * 1024 * 1024
        ),
        cost_estimate=pl.CostEstimate(
            flops=16 * BS * BS * SHARE, bytes_accessed=16 * BS * BS, transcendentals=0
        ),
    )(table, grad, left, right)


def finish_kernel(
    left_stat, right_stat, left_term, right_term, home, positions_in, keep,
    left_next, right_next, update_out,
    left_new, right_new, positions, sem,
):
    load = pltpu.make_async_copy(positions_in, positions, sem.at[0])
    load.start()
    copies = []

    def next_of(s, stat, term, new, out, part):
        rows = pl.ds(part * (BS // 2), BS // 2)
        new[s, rows] = keep[s][:1, :1] * stat[s, rows] + (1.0 - decay_rate) * f32(term[s, rows])
        copy = pltpu.make_async_copy(new.at[s, rows], out.at[s, rows], sem.at[2 + len(copies)])
        copy.start()
        copies.append(copy)

    sides = (
        (left_stat, left_term, left_new, left_next),
        (right_stat, right_term, right_new, right_next),
    )
    parts = [(s, side, part) for s in range(2) for side in sides for part in range(2)]
    placed = 0
    for k, (s, side, part) in enumerate(parts):
        next_of(s, *side, part)
        if k == 1:
            load.wait()
        if k >= 1:
            upto = BLOCKS * k // (len(parts) - 1)
            for b in range(placed, upto):
                pltpu.make_async_copy(home.at[positions[0, b]], update_out.at[b], sem.at[1]).start()
            placed = upto
    for copy in copies:
        copy.wait()
    wait_for(update_out, sem.at[1])


def finish(*operands):
    vmem_spec = pl.BlockSpec(memory_space=pltpu.VMEM)
    any_spec = pl.BlockSpec(memory_space=pl.ANY)
    stat_shape = jax.ShapeDtypeStruct((2, BS, SHARE), jnp.float32)
    return pl.pallas_call(
        finish_kernel,
        name="shampoo_finish",
        out_shape=(
            stat_shape, stat_shape, jax.ShapeDtypeStruct((BLOCKS, ROWS, SHARE), jnp.bfloat16)
        ),
        in_specs=[vmem_spec] * 4 + [any_spec] * 2 + [vmem_spec],
        out_specs=(any_spec,) * 3,
        scratch_shapes=[
            pltpu.VMEM((2, BS, SHARE), jnp.float32),
            pltpu.VMEM((2, BS, SHARE), jnp.float32),
            pltpu.SMEM((1, LANES), jnp.int32),
            pltpu.SemaphoreType.DMA((10,)),
        ],
        compiler_params=pltpu.CompilerParams(vmem_limit_bytes=24 * 1024 * 1024),
        cost_estimate=pl.CostEstimate(flops=4 * BS * BS, bytes_accessed=8 * BS * BS, transcendentals=0),
    )(*operands)


def on_device(partial_grad, owner_table, left_stat, right_stat, left_root, right_root):
    left_term, right_term, home, positions, keep = exchange(
        owner_table.T,
        partial_grad[0],
        left_root[0].reshape(2, NZ, LANES, SHARE),
        right_root[0],
    )

    left_next, right_next, update = finish(
        left_stat[0], right_stat[0], left_term, right_term, home, positions, keep
    )
    return left_next[None], right_next[None], update


def solution(mesh):
    return jax.shard_map(
        on_device,
        mesh=mesh,
        in_specs=(
            P("rep", None, "fsdp", None),
            P(),
            P("fsdp", None, None, "rep"),
            P("fsdp", None, None, "rep"),
            P("fsdp", None, None, "rep"),
            P("fsdp", None, None, "rep"),
        ),
        out_specs=(
            P("fsdp", None, None, "rep"),
            P("fsdp", None, None, "rep"),
            P(None, "fsdp", "rep"),
        ),
        check_vma=False,
    )
```
